128 devices in a mesh: segment: 2 (over core), grp: 64 (over x, z, y).
Axes of the slice: x: 4, y: 4, z: 4, core: 2. Of those that a mesh axis runs over, the one named last changes fastest.
Arguments:
- monomer_density: bfloat16 [512, 9216], P('grp'), may hold values from -3 to 3
- monomer_centers: float32 [3, 512], replicated, may hold values from 0 to 8
- dimer_pairs: int32 [2, 1024], replicated, may hold values from 0 to 511, as said below
- basis_sizes: int32 [512], replicated, may hold values from 48 to 96
- dimer_core: float32 [1024, 36864], P('grp')
- esp_map: float32 [96, 192], replicated, may hold values from -0.1875 to 0.1875
- repulsion: float32 [36864], replicated, may hold values from 0.005 to 0.05
Outputs:
- section_out: float32 [2, 1024, 36864], P('segment', 'grp')
- window_energy: float32 [], replicated
The draws below stay inside these ranges and needn't reach their ends.
Inputs may be any that keep to these rules, and one draw needn't show every extreme that they name: `dimer_pairs`: the two monomers of a dimer differ.
All inputs are finite; a program needn't handle non-finite values. Where the reference program divides by a largest or mean magnitude, that divisor is 1e-20 or more.
Results may differ from the reference program's by a relative error of at most 0.00045.
Values may be sent and summed in bfloat16 or wider, within the bound.
No kernel may reach another device: no remote copies, remote signals or barrier semaphores. Data moves between devices by JAX's collectives and lax.ppermute only.
A program may use at most 128 MiB of HBM per device.

```python
import jax
import jax.numpy as jnp
from jax import lax

BM = 96
BD = 192
SCF_ITERS = 1
PURIFY = 8
DIMS_DEV = 16
NMON = 512
NDIM = 1024


def draw_dimer_pairs(key, part):
    first_key, second_key = jax.random.split(jax.random.fold_in(key, 11))
    first_ids = jax.random.randint(first_key, (NDIM,), 0, NMON)
    offsets = jax.random.randint(second_key, (NDIM,), 1, NMON)
    second_ids = (first_ids + offsets) % NMON
    return jnp.stack([first_ids, second_ids]).astype(jnp.int32)


def draw_dimer_core(key, part):
    base_key, onsite_key = jax.random.split(jax.random.fold_in(key, 23), 2)
    coupling = 0.15 * jax.random.normal(base_key, (NDIM, BD, BD), jnp.float32)
    onsite = jax.random.uniform(onsite_key, (NDIM, BD), jnp.float32, -1.5, 1.5)
    identity = jnp.eye(BD, dtype=jnp.float32)
    square = coupling + onsite[:, :, None] * identity
    return square.reshape(NDIM, BD * BD).astype(jnp.float32)


def plant(entries, own_key, smallest, largest):
    extent = entries.shape
    place = [jax.random.randint(jax.random.fold_in(own_key, axis), (), 0, extent[axis]) for axis in range(len(extent))]
    entries = entries.at[tuple(place)].set(smallest)
    longest = extent.index(max(extent))
    place[longest] = (place[longest] + 1) % extent[longest]
    return entries.at[tuple(place)].set(largest)


def shard_levels(own_key, dims, shards, least, high):
    level = 1.0
    for dim, parts in shards:
        steps = jax.random.uniform(jax.random.fold_in(jax.random.fold_in(own_key, 6), dim), (parts,), jnp.float32, least / len(shards), high / len(shards))
        level = level * jnp.repeat(jnp.exp(steps), dims[dim] // parts).reshape((-1,) + (1,) * (len(dims) - 1 - dim))
    return level


def scatter_about(own_key, dims, deviation, bound, shards=(), kind=jnp.bfloat16):
    factor_of = shard_levels(own_key, dims, shards, -0.22, 0.18) if shards else 1.0
    result = jax.random.normal(own_key, dims, jnp.float32) * deviation * factor_of
    return jnp.minimum(jnp.maximum(result, -bound), bound).astype(kind)


def setup_inputs(seed: int = 0) -> dict:
    splits = jax.random.split(jax.random.key(seed), 8)
    return {
        "monomer_density": scatter_about(splits[0], (NMON, BM * BM), 0.5, 3.0, ((0, 64),)),
        "monomer_centers": jnp.clip(jax.random.uniform(splits[1], (3, NMON), jnp.float32, 0.0, 8.0), 0.0, 8.0),
        "dimer_pairs": draw_dimer_pairs(jax.random.fold_in(splits[7], 71), 0),
        "basis_sizes": plant(jax.random.randint(splits[3], (NMON,), BM // 2, BM + 1), jax.random.fold_in(splits[3], 1), BM // 2, BM).astype(jnp.int32),
        "dimer_core": draw_dimer_core(jax.random.fold_in(splits[7], 71), 0),
        "esp_map": scatter_about(splits[5], (BM, BD), (BM * 12) ** -0.5, 0.1875, (), jnp.float32),
        "repulsion": jnp.clip(jax.random.uniform(splits[6], (BD * BD,), jnp.float32, 0.005, 0.05), 0.005, 0.05),
    }


epsilon = 1e-06
highest = lax.Precision.HIGHEST

def esp_weights(first_ids, second_ids, centers, first_row, row_count):
    nearby = lax.dynamic_slice_in_dim(centers, first_row, row_count, 1)
    middle = 0.5 * (centers[:, first_ids] + centers[:, second_ids])
    distance = jnp.zeros((first_ids.shape[0], row_count), jnp.float32)
    for axis_pos in range(3):
        axis_gap = middle[axis_pos][:, None] - nearby[axis_pos][None, :]
        distance = distance + axis_gap * axis_gap
    weights = 1.0 / jnp.sqrt(distance + 1.0)
    labels = first_row + jnp.arange(row_count, dtype=jnp.int32)
    excluded = (labels[None, :] == first_ids[:, None]) | (labels[None, :] == second_ids[:, None])
    return jnp.where(excluded, 0.0, weights)

def live_masks(first_ids, second_ids, basis_sizes, width):
    first_size = basis_sizes[first_ids]
    second_size = basis_sizes[second_ids]
    position = jnp.arange(2 * width, dtype=jnp.int32)
    inside = jnp.where(position[None, :] < width, position[None, :] < first_size[:, None], position[None, :] - width < second_size[:, None])
    return inside.astype(jnp.float32)

def embedded(field_sum, core_rows, esp_map):
    row_count = core_rows.shape[0]
    width = esp_map.shape[0]
    field = field_sum.reshape(row_count, width, width)
    field = 0.5 * (field + jnp.swapaxes(field, 1, 2))
    left_side = jnp.einsum('am,kab->kmb', esp_map, field, precision=highest)
    potential = jnp.einsum('kmb,bn->kmn', left_side, esp_map, precision=highest)
    return 0.5 * (core_rows + jnp.swapaxes(core_rows, 1, 2)) + potential

def purify(fock_matrix, live_mask):
    pair_mask = live_mask[:, :, None] * live_mask[:, None, :]
    masked = fock_matrix * pair_mask
    identity = jnp.eye(fock_matrix.shape[1], dtype=jnp.float32)
    live_diag = live_mask[:, :, None] * identity
    chemical = lax.optimization_barrier(jnp.sum(masked * identity, axis=(1, 2))) / lax.optimization_barrier(jnp.sum(live_mask, axis=1))
    shifted = masked - chemical[:, None, None] * live_diag
    radius = lax.optimization_barrier(jnp.max(lax.optimization_barrier(jnp.sum(jnp.abs(shifted), axis=2)), axis=1))
    scaling = 0.5 / (radius + epsilon)
    density = 0.5 * live_diag - scaling[:, None, None] * shifted
    for repeat in range(PURIFY):
        squared = jnp.einsum('kab,kbc->kac', density, density, precision=highest)
        density = 3.0 * squared - 2.0 * jnp.einsum('kab,kbc->kac', squared, density, precision=highest)
    return density

def fock_update(core_fock, density, repulsion):
    symmetric = 0.5 * (repulsion + repulsion.T)
    occupied = jnp.diagonal(density, axis1=1, axis2=2)
    coulomb = jnp.dot(occupied, symmetric, precision=highest)
    identity = jnp.eye(density.shape[1], dtype=jnp.float32)
    return core_fock + coulomb[:, :, None] * identity - 0.5 * symmetric[None] * density

def scf_solve(core_fock, live_mask, repulsion):
    density = purify(core_fock, live_mask)
    fock_matrix = core_fock
    for repeat in range(SCF_ITERS):
        fock_matrix = fock_update(core_fock, density, repulsion)
        density = purify(fock_matrix, live_mask)
    energy = 0.5 * lax.optimization_barrier(jnp.sum(density * (core_fock + fock_matrix), axis=(1, 2))) / lax.optimization_barrier(jnp.sum(live_mask, axis=1))
    return (density, energy)

def reference(monomer_density, monomer_centers, dimer_pairs, basis_sizes, dimer_core, esp_map, repulsion):
    monomers = monomer_density.shape[0]
    width = esp_map.shape[0]
    full = esp_map.shape[1]
    first_ids = dimer_pairs[0].astype(jnp.int32)
    second_ids = dimer_pairs[1].astype(jnp.int32)
    weights = esp_weights(first_ids, second_ids, monomer_centers, jnp.int32(0), monomers).astype(jnp.bfloat16)
    field_sum = jnp.dot(weights, monomer_density, preferred_element_type=jnp.float32)
    core_square = dimer_core.reshape(dimer_core.shape[0], full, full)
    repulsion_square = repulsion.reshape(full, full)
    core_fock = embedded(field_sum, core_square, esp_map)
    live_mask = live_masks(first_ids, second_ids, basis_sizes, width)
    groups = core_fock.shape[0] // DIMS_DEV

    def solve_group(operands):
        return scf_solve(operands[0], operands[1], repulsion_square)
    density, energy = lax.map(solve_group, (core_fock.reshape(groups, DIMS_DEV, full, full), live_mask.reshape(groups, DIMS_DEV, full)))
    section_out = jnp.stack([core_fock.reshape(-1, full * full), density.reshape(-1, full * full)])
    window_energy = jnp.sum(energy) / core_fock.shape[0]
    return (section_out, window_energy)
```

```python
import jax
import jax.numpy as jnp
from jax import lax
from jax.experimental import pallas as pl
from jax.experimental.pallas import tpu as pltpu
from jax.sharding import Mesh
from jax.sharding import PartitionSpec as P


PURIFY = 8
PASSES = (3, 3)
GRP = ("grp_0", "grp_1", "grp_2")
ALL = ("segment", "grp_0", "grp_1", "grp_2")
STRIDES = ((1, 4, 16), (4, 16, 1))

BM = 96
BD = 192
FLAT = BD * BD
TILES = FLAT // 128
HALF = BM * BM // 2
LOCAL = 8
PITCH = 292
FPITCH = 73
epsilon = 1e-06
highest = lax.Precision.HIGHEST
f32 = jnp.float32
bf16 = jnp.bfloat16


def phase_shift(value, phase, step):
    pairs = []
    for core in range(2):
        stride = STRIDES[core][phase]
        for chip in range(64):
            place = (chip // stride) % 4
            target = chip + (((place + step) % 4) - place) * stride
            pairs.append((core * 64 + chip, core * 64 + target))
    return lax.ppermute(value, ALL, pairs)


def axis_shift(value, axis, step):
    return lax.ppermute(value, axis, [(i, (i + step) % 4) for i in range(4)])


def swap_cores(value):
    return lax.ppermute(value, "segment", [(0, 1), (1, 0)])


def split_two(value):
    high = value.astype(bf16)
    low = (value - high.astype(f32)).astype(bf16)
    return high, low


def dot(left, right):
    return jnp.dot(left, right, preferred_element_type=f32)


def dot_three(left, right):
    (lh, ll), (rh, rl) = left, right
    return dot(lh, rh) + (dot(ll, rh) + dot(lh, rl))


def lane_index(rows):
    return lax.broadcasted_iota(jnp.int32, (rows, 128), 1)


def unflatten_kernel(segment_ref, core_ref, first_ref, second_ref, flat):
    for tile in range(TILES):
        flat[pl.ds(tile, LOCAL, stride=PITCH), :] = core_ref[:, tile * 128 : tile * 128 + 128]
    low_half = lane_index(BM) < 64
    for d in range(LOCAL):
        a = flat[pl.ds(d * PITCH, BM, stride=3), :]
        b = flat[pl.ds(d * PITCH + 1, BM, stride=3), :]
        c = flat[pl.ds(d * PITCH + 2, BM, stride=3), :]
        b_rolled = pltpu.roll(b, 64, 1)
        c_rolled = pltpu.roll(c, 64, 1)
        first_ref[pl.ds(d * BD, BM, stride=2), :] = a
        second_ref[pl.ds(d * BD, BM, stride=2), :] = b
        first_ref[pl.ds(d * BD + 1, BM, stride=2), :] = jnp.where(low_half, b_rolled, c_rolled)
        second_ref[pl.ds(d * BD + 1, BM, stride=2), :] = c_rolled


def unflatten(segment, core):
    return pl.pallas_call(
        unflatten_kernel,
        name="unflatten",
        grid_spec=pltpu.PrefetchScalarGridSpec(
            num_scalar_prefetch=1,
            grid=(1,),
            in_specs=[pl.BlockSpec((LOCAL, FLAT), lambda i, s: (s[0], 0))],
            out_specs=[pl.BlockSpec((LOCAL * BD, 128), lambda i, s: (0, 0))] * 2,
            scratch_shapes=[pltpu.VMEM((LOCAL * PITCH, 128), f32)],
        ),
        out_shape=[jax.ShapeDtypeStruct((LOCAL * BD, 128), f32)] * 2,
        cost_estimate=pl.CostEstimate(flops=20000000, bytes_accessed=3000000, transcendentals=0),
    )(segment, core)


def flatten_kernel(square_ref, out_ref, first, second, flat):
    low_half = lane_index(BM) < 64
    for d in range(LOCAL):
        first[...] = square_ref[d, :, 0:128]
        second[:, 0:64] = square_ref[d, :, 128:192]
        even_a = first[pl.ds(0, BM, stride=2), :]
        even_b = second[pl.ds(0, BM, stride=2), :]
        odd_a = pltpu.roll(first[pl.ds(1, BM, stride=2), :], 64, 1)
        odd_b = pltpu.roll(second[pl.ds(1, BM, stride=2), :], 64, 1)
        flat[pl.ds(d * PITCH, BM, stride=3), :] = even_a
        flat[pl.ds(d * PITCH + 1, BM, stride=3), :] = jnp.where(low_half, even_b, odd_a)
        flat[pl.ds(d * PITCH + 2, BM, stride=3), :] = jnp.where(low_half, odd_a, odd_b)
    for tile in range(TILES):
        out_ref[:, tile * 128 : tile * 128 + 128] = flat[pl.ds(tile, LOCAL, stride=PITCH), :]


def flatten(square):
    return pl.pallas_call(
        flatten_kernel,
        name="flatten",
        out_shape=jax.ShapeDtypeStruct((LOCAL, FLAT), f32),
        scratch_shapes=[
            pltpu.VMEM((BD, 128), f32),
            pltpu.VMEM((BD, 128), f32),
            pltpu.VMEM((LOCAL * PITCH, 128), f32),
        ],
        cost_estimate=pl.CostEstimate(flops=20000000, bytes_accessed=3000000, transcendentals=0),
    )(square)


def partial_kernel(weight_ref, b0, b1, b2, b3, o0, o1, o2, o3):
    for start in range(0, HALF, 512):
        columns = slice(start, start + 512)
        rows = jnp.concatenate([b[:, columns] for b in (b0, b1, b2, b3)], axis=0)
        total = dot(weight_ref[...], rows)
        for k, out in enumerate((o0, o1, o2, o3)):
            out[:, columns] = total[16 * k : 16 * k + 16]


def partial_fields(weights, blocks):
    return pl.pallas_call(
        partial_kernel,
        name="partial_fields",
        out_shape=[jax.ShapeDtypeStruct((16, HALF), f32)] * 4,
        cost_estimate=pl.CostEstimate(flops=80000000, bytes_accessed=2400000, transcendentals=0),
    )(weights, *blocks)


def live_square(n_first, n_second):
    row = lax.broadcasted_iota(jnp.int32, (BD, BD), 0)
    column = lax.broadcasted_iota(jnp.int32, (BD, BD), 1)

    def inside(position):
        limit = jnp.where(position < BM, n_first, n_second + BM)
        return position < limit

    live = jnp.logical_and(inside(row), inside(column))
    return live, row == column


def solve_kernel(
    segment_ref, sizes_ref, mine_ref, theirs_ref, first_ref, second_ref, esp_ref, esp_t_ref, rep_ref,
    core_out, density_out, energy_out,
    flat, field, fock, work, work_h, work_l, square_h, square_l, diagonals,
):
    segment = segment_ref[0]
    own_start = 36 * segment
    other_start = 36 - own_start
    for tile in range(36):
        columns = slice(tile * 128, tile * 128 + 128)
        flat[pl.ds(own_start + tile, LOCAL, stride=FPITCH), :] = mine_ref[:, columns]
        flat[pl.ds(other_start + tile, LOCAL, stride=FPITCH), :] = theirs_ref[:, columns]
    esp = split_two(esp_ref[...])
    esp_t = split_two(esp_t_ref[...])
    repulsion = 0.5 * (rep_ref[...] + rep_ref[...].T)
    lane = lane_index(24)
    for d in range(LOCAL):
        a = flat[pl.ds(d * FPITCH, 24, stride=3), :]
        b = flat[pl.ds(d * FPITCH + 1, 24, stride=3), :]
        c = flat[pl.ds(d * FPITCH + 2, 24, stride=3), :]
        base = d * BM
        field[pl.ds(base, 24, stride=4), :] = a
        field[pl.ds(base + 1, 24, stride=4), :] = jnp.where(
            lane < 32, pltpu.roll(a, 32, 1), pltpu.roll(b, 32, 1)
        )
        field[pl.ds(base + 2, 24, stride=4), :] = jnp.where(
            lane < 64, pltpu.roll(b, 64, 1), pltpu.roll(c, 64, 1)
        )
        field[pl.ds(base + 3, 24, stride=4), :] = pltpu.roll(c, 96, 1)
    for d in range(LOCAL):
        left = dot_three(esp_t, split_two(field[d * BM : d * BM + BM, 0:BM]))
        potential = dot_three(split_two(left), esp)
        rows = slice(d * BD, d * BD + BD)
        core = jnp.concatenate([first_ref[rows, :], second_ref[rows, 0:64]], axis=1)
        total = core + potential
        core_out[d] = 0.5 * (total + total.T)

    def live_count(d):
        n_first = jnp.clip(sizes_ref[0, d], 0, BM)
        n_second = jnp.clip(sizes_ref[1, d], 0, BM)
        return n_first, n_second, (n_first + n_second).astype(f32)

    def purify(source, passes):
        for d in range(LOCAL):
            n_first, n_second, count = live_count(d)
            live, diagonal = live_square(n_first, n_second)
            masked = jnp.where(live, source[d], 0.0)
            on_diagonal = jnp.logical_and(live, diagonal)
            chemical = jnp.sum(jnp.where(diagonal, masked, 0.0)) / count
            shifted = masked - jnp.where(on_diagonal, chemical, 0.0)
            radius = jnp.max(jnp.sum(jnp.abs(shifted), axis=0, keepdims=True))
            work[d] = shifted * (-0.5 / (radius + epsilon))

        def step(_, carry):
            for d in range(LOCAL):
                high, low = split_two(work[d])
                work_h[d] = high
                if passes == 3:
                    work_l[d] = low
                    squared = dot_three((high, low), (high, low))
                    square_h[d], square_l[d] = split_two(squared)
                else:
                    square_h[d] = dot(high, high).astype(bf16)
            for d in range(LOCAL):
                if passes == 3:
                    cubed = dot_three((square_h[d], square_l[d]), (work_h[d], work_l[d]))
                else:
                    cubed = dot(square_h[d], work_h[d])
                work[d] = 1.5 * work[d] - 2.0 * cubed
            return carry

        lax.fori_loop(0, PURIFY, step, 0)

    def density_of(d):
        n_first, n_second, count = live_count(d)
        live, diagonal = live_square(n_first, n_second)
        return work[d] + jnp.where(jnp.logical_and(live, diagonal), 0.5, 0.0), diagonal, count

    purify(core_out, PASSES[0])
    for d in range(LOCAL):
        density, diagonal, _ = density_of(d)
        diagonals[d : d + 1, :] = jnp.sum(jnp.where(diagonal, density, 0.0), axis=0, keepdims=True)
    coulomb = jnp.dot(diagonals[...], repulsion, precision=highest, preferred_element_type=f32)
    for d in range(LOCAL):
        density, diagonal, _ = density_of(d)
        fock[d] = (
            core_out[d]
            + jnp.where(diagonal, coulomb[d : d + 1, :], 0.0)
            - 0.5 * (repulsion * density)
        )
    purify(fock, PASSES[1])
    energy = jnp.zeros((1, BD), f32)
    for d in range(LOCAL):
        density, _, count = density_of(d)
        density_out[d] = density
        terms = jnp.sum(density * (core_out[d] + fock[d]), axis=0, keepdims=True)
        energy = energy + terms * (0.5 / count)
    energy_out[...] = jnp.full((8, 128), jnp.sum(energy), f32)


def solve(segment, sizes, mine, theirs, first, second, esp_map, repulsion):
    vmem = pl.BlockSpec(memory_space=pltpu.VMEM)
    smem = pl.BlockSpec(memory_space=pltpu.SMEM)
    square = (LOCAL, BD, BD)
    return pl.pallas_call(
        solve_kernel,
        name="solve",
        in_specs=[smem, smem] + [vmem] * 7,
        out_specs=[vmem] * 3,
        out_shape=[
            jax.ShapeDtypeStruct(square, f32),
            jax.ShapeDtypeStruct(square, f32),
            jax.ShapeDtypeStruct((8, 128), f32),
        ],
        scratch_shapes=[
            pltpu.VMEM((LOCAL * FPITCH, 128), f32),
            pltpu.VMEM((LOCAL * BM, 128), f32),
            pltpu.VMEM(square, f32),
            pltpu.VMEM(square, f32),
            pltpu.VMEM(square, bf16),
            pltpu.VMEM(square, bf16),
            pltpu.VMEM(square, bf16),
            pltpu.VMEM(square, bf16),
            pltpu.VMEM((LOCAL, BD), f32),
        ],
        cost_estimate=pl.CostEstimate(
            flops=11000000000, bytes_accessed=6000000, transcendentals=0
        ),
    )(segment, sizes, mine, theirs, first, second, esp_map, esp_map.T, repulsion)


def esp_weights(first_ids, second_ids, centers, labels):
    middle = 0.5 * (centers[:, first_ids] + centers[:, second_ids])
    nearby = centers[:, labels]
    distance = jnp.zeros((first_ids.shape[0], labels.shape[0]), f32)
    for axis_pos in range(3):
        axis_gap = middle[axis_pos][:, None] - nearby[axis_pos][None, :]
        distance = distance + axis_gap * axis_gap
    weights = 1.0 / jnp.sqrt(distance + 1.0)
    excluded = (labels[None, :] == first_ids[:, None]) | (labels[None, :] == second_ids[:, None])
    return jnp.where(excluded, 0.0, weights)


def on_device(
    monomer_density, monomer_centers, dimer_pairs, basis_sizes, dimer_core, esp_map, repulsion
):
    chip = lax.axis_index(GRP)
    segment = lax.axis_index("segment")
    segment_array = segment.reshape(1).astype(jnp.int32)

    own = lax.dynamic_slice_in_dim(monomer_density, segment * HALF, HALF, 1)
    gathered = jnp.concatenate([own] + [phase_shift(own, 0, k) for k in (1, 2, 3)], axis=0)
    blocks = [gathered] + [phase_shift(gathered, 1, k) for k in (1, 2, 3)]

    strides = [jnp.where(segment == 0, STRIDES[0][p], STRIDES[1][p]) for p in range(3)]
    places = [(chip // strides[p]) % 4 for p in range(3)]

    def moved(chips, phase, step):
        return chips + ((places[phase] + step + 4) % 4 - places[phase]) * strides[phase]

    steps = jnp.arange(4, dtype=jnp.int32)
    targets = moved(chip, 2, steps)
    dimers = (targets[:, None] * 16 + jnp.arange(16, dtype=jnp.int32)[None, :]).reshape(64)
    sources = moved(moved(chip, 0, -steps)[None, :], 1, -steps[:, None])
    labels = (sources[:, :, None] * 8 + jnp.arange(8, dtype=jnp.int32)).reshape(128)
    pairs = dimer_pairs[:, dimers]
    weights = esp_weights(pairs[0], pairs[1], monomer_centers, labels).astype(bf16)

    first, second = unflatten(segment_array, dimer_core)
    own_pairs = lax.dynamic_slice_in_dim(dimer_pairs, chip * 16 + segment * 8, 8, 1)
    sizes = basis_sizes[own_pairs]
    square_repulsion = repulsion.reshape(BD, BD)

    parts = partial_fields(weights, blocks)
    total = parts[0]
    for k in (1, 2, 3):
        total = total + phase_shift(parts[k], 2, k)
    mine = lax.dynamic_slice_in_dim(total, segment * 8, 8, 0)
    theirs = swap_cores(lax.dynamic_slice_in_dim(total, (1 - segment) * 8, 8, 0))

    core_fock, density, energy = solve(
        segment_array, sizes, mine, theirs, first, second, esp_map, square_repulsion
    )

    for axis in GRP:
        one, two, three = [axis_shift(energy, axis, k) for k in (1, 2, 3)]
        energy = (energy + two) + (one + three)
    energy = energy + swap_cores(energy)
    window_energy = energy[0, 0] / 1024.0

    is_first = segment == 0
    flat_core = flatten(core_fock)
    flat_density = flatten(density)
    arrived = swap_cores(jnp.where(is_first, flat_density, flat_core))
    keeping = jnp.where(is_first, flat_core, flat_density)
    lower = jnp.where(is_first, keeping, arrived)
    upper = jnp.where(is_first, arrived, keeping)
    return (jnp.concatenate([lower, upper], axis=0)[None], window_energy)


def solution(mesh):
    split = Mesh(
        mesh.devices.reshape(mesh.shape["segment"], 4, 4, 4), ("segment", "grp_0", "grp_1", "grp_2")
    )
    return jax.shard_map(
        on_device,
        mesh=split,
        in_specs=(P(GRP, None), P(), P(), P(), P(GRP, None), P(), P()),
        out_specs=(P("segment", GRP, None), P()),
        check_vma=False,
    )
```

```python
import jax
import jax.numpy as jnp
from jax import lax
from jax.experimental import pallas as pl
from jax.experimental.pallas import tpu as pltpu
from jax.sharding import Mesh
from jax.sharding import PartitionSpec as P


PURIFY = 8
SINGLE = (8, 4)
MIB = 1024 * 1024
GRP = ("grp_0", "grp_1", "grp_2")
ALL = ("segment", "grp_0", "grp_1", "grp_2")
STRIDES = ((1, 4, 16), (4, 16, 1))

BM = 96
BD = 192
FLAT = BD * BD
TILES = FLAT // 128
HALF = BM * BM // 2
LOCAL = 8
PITCH = 292
FPITCH = 73
epsilon = 1e-06
highest = lax.Precision.HIGHEST
f32 = jnp.float32
bf16 = jnp.bfloat16


def phase_shift(value, phase, step):
    pairs = []
    for core in range(2):
        stride = STRIDES[core][phase]
        for chip in range(64):
            place = (chip // stride) % 4
            target = chip + (((place + step) % 4) - place) * stride
            pairs.append((core * 64 + chip, core * 64 + target))
    return lax.ppermute(value, ALL, pairs)


def shifts(shift, *args):
    arrived = []
    for step in (1, 2, 3):
        arrived.append(shift(*args, step))
    return arrived


def axis_shift(value, axis, step):
    return lax.ppermute(value, axis, [(i, (i + step) % 4) for i in range(4)])


def swap_cores(value):
    return lax.ppermute(value, "segment", [(0, 1), (1, 0)])


def split_two(value):
    high = value.astype(bf16)
    low = (value - high.astype(f32)).astype(bf16)
    return high, low


def dot(left, right):
    return jnp.dot(left, right, preferred_element_type=f32)


def dot_three(left, right):
    (lh, ll), (rh, rl) = left, right
    return dot(lh, rh) + (dot(ll, rh) + dot(lh, rl))


def lane_index(rows):
    return lax.broadcasted_iota(jnp.int32, (rows, 128), 1)


def unflatten_kernel(segment_ref, core_ref, first_ref, second_ref, flat):
    for tile in range(TILES):
        flat[pl.ds(tile, LOCAL, stride=PITCH), :] = core_ref[:, tile * 128 : tile * 128 + 128]
    low_half = lane_index(BM) < 64
    for d in range(LOCAL):
        a = flat[pl.ds(d * PITCH, BM, stride=3), :]
        b = flat[pl.ds(d * PITCH + 1, BM, stride=3), :]
        c = flat[pl.ds(d * PITCH + 2, BM, stride=3), :]
        b_rolled = pltpu.roll(b, 64, 1)
        c_rolled = pltpu.roll(c, 64, 1)
        first_ref[pl.ds(d * BD, BM, stride=2), :] = a
        second_ref[pl.ds(d * BD, BM, stride=2), :] = b
        first_ref[pl.ds(d * BD + 1, BM, stride=2), :] = jnp.where(low_half, b_rolled, c_rolled)
        second_ref[pl.ds(d * BD + 1, BM, stride=2), :] = c_rolled


def unflatten(segment, core):
    return pl.pallas_call(
        unflatten_kernel,
        name="unflatten",
        grid_spec=pltpu.PrefetchScalarGridSpec(
            num_scalar_prefetch=1,
            grid=(1,),
            in_specs=[pl.BlockSpec((LOCAL, FLAT), lambda i, s: (s[0], 0))],
            out_specs=[pl.BlockSpec((LOCAL * BD, 128), lambda i, s: (0, 0))] * 2,
            scratch_shapes=[pltpu.VMEM((LOCAL * PITCH, 128), f32)],
        ),
        out_shape=[jax.ShapeDtypeStruct((LOCAL * BD, 128), f32)] * 2,
        cost_estimate=pl.CostEstimate(flops=20000000, bytes_accessed=3000000, transcendentals=0),
    )(segment, core)


def flatten_kernel(place_ref, square_ref, out_ref, first, second, flat):
    low_half = lane_index(BM) < 64
    for d in range(LOCAL):
        first[...] = square_ref[0, d, :, 0:128]
        second[:, 0:64] = square_ref[0, d, :, 128:192]
        even_a = first[pl.ds(0, BM, stride=2), :]
        even_b = second[pl.ds(0, BM, stride=2), :]
        odd_a = pltpu.roll(first[pl.ds(1, BM, stride=2), :], 64, 1)
        odd_b = pltpu.roll(second[pl.ds(1, BM, stride=2), :], 64, 1)
        flat[pl.ds(d * PITCH, BM, stride=3), :] = even_a
        flat[pl.ds(d * PITCH + 1, BM, stride=3), :] = jnp.where(low_half, even_b, odd_a)
        flat[pl.ds(d * PITCH + 2, BM, stride=3), :] = jnp.where(low_half, odd_a, odd_b)
    for tile in range(TILES):
        out_ref[:, tile * 128 : tile * 128 + 128] = flat[pl.ds(tile, LOCAL, stride=PITCH), :]


def flatten(place, stack, rows):
    return pl.pallas_call(
        flatten_kernel,
        name="flatten",
        grid_spec=pltpu.PrefetchScalarGridSpec(
            num_scalar_prefetch=1,
            grid=(1,),
            in_specs=[pl.BlockSpec((1, LOCAL, BD, BD), lambda i, p: (p[0], 0, 0, 0))],
            out_specs=pl.BlockSpec((LOCAL, FLAT), lambda i, p: (p[1], 0)),
            scratch_shapes=[
                pltpu.VMEM((BD, 128), f32),
                pltpu.VMEM((BD, 128), f32),
                pltpu.VMEM((LOCAL * PITCH, 128), f32),
            ],
        ),
        out_shape=jax.ShapeDtypeStruct((rows, FLAT), f32),
        cost_estimate=pl.CostEstimate(flops=20000000, bytes_accessed=3000000, transcendentals=0),
    )(place, stack)


def partial_kernel(weight_ref, b0, b1, b2, b3, o0, o1, o2, o3):
    for start in range(0, HALF, 512):
        columns = slice(start, start + 512)
        rows = jnp.concatenate([b[:, columns] for b in (b0, b1, b2, b3)], axis=0)
        total = dot(weight_ref[...], rows)
        for k, out in enumerate((o0, o1, o2, o3)):
            out[:, columns] = total[16 * k : 16 * k + 16]


def partial_fields(weights, blocks):
    return pl.pallas_call(
        partial_kernel,
        name="partial_fields",
        out_shape=[pltpu.HBM((16, HALF), f32)] * 4,
        compiler_params=pltpu.CompilerParams(vmem_limit_bytes=12 * MIB),
        cost_estimate=pl.CostEstimate(flops=80000000, bytes_accessed=2400000, transcendentals=0),
    )(weights, *blocks)


def live_square(n_first, n_second):
    row = lax.broadcasted_iota(jnp.int32, (BD, BD), 0)
    column = lax.broadcasted_iota(jnp.int32, (BD, BD), 1)

    def inside(position):
        limit = jnp.where(position < BM, n_first, n_second + BM)
        return position < limit

    live = jnp.logical_and(inside(row), inside(column))
    return live, row == column


def solve_kernel(
    segment_ref, sizes_ref, mine_any, theirs_any, first_any, second_any, esp_any, rep_any,
    stack, energy_out,
    mine_ref, theirs_ref, first_ref, second_ref, esp_ref, rep_ref, arrivals,
    flat, field, fock, work, work_h, work_l, square_h, square_l, diagonals,
):
    places = (
        (mine_any, mine_ref), (theirs_any, theirs_ref), (esp_any, esp_ref),
        (first_any, first_ref), (second_any, second_ref), (rep_any, rep_ref),
    )
    copies = [
        pltpu.make_async_copy(source, target, arrivals.at[i])
        for i, (source, target) in enumerate(places)
    ]
    for copy in copies:
        copy.start()
    copies[0].wait()
    copies[1].wait()
    core_out = stack.at[0]
    density_out = stack.at[1]
    segment = segment_ref[0]
    own_start = 36 * segment
    other_start = 36 - own_start
    for tile in range(36):
        columns = slice(tile * 128, tile * 128 + 128)
        flat[pl.ds(own_start + tile, LOCAL, stride=FPITCH), :] = mine_ref[:, columns]
        flat[pl.ds(other_start + tile, LOCAL, stride=FPITCH), :] = theirs_ref[:, columns]
    for copy in copies[2:]:
        copy.wait()
    esp = split_two(esp_ref[...])
    esp_t = split_two(esp_ref[...].T)
    repulsion = 0.5 * (rep_ref[...] + rep_ref[...].T)
    lane = lane_index(24)
    for d in range(LOCAL):
        a = flat[pl.ds(d * FPITCH, 24, stride=3), :]
        b = flat[pl.ds(d * FPITCH + 1, 24, stride=3), :]
        c = flat[pl.ds(d * FPITCH + 2, 24, stride=3), :]
        base = d * BM
        field[pl.ds(base, 24, stride=4), :] = a
        field[pl.ds(base + 1, 24, stride=4), :] = jnp.where(
            lane < 32, pltpu.roll(a, 32, 1), pltpu.roll(b, 32, 1)
        )
        field[pl.ds(base + 2, 24, stride=4), :] = jnp.where(
            lane < 64, pltpu.roll(b, 64, 1), pltpu.roll(c, 64, 1)
        )
        field[pl.ds(base + 3, 24, stride=4), :] = pltpu.roll(c, 96, 1)
    for d in range(LOCAL):
        left = dot_three(esp_t, split_two(field[d * BM : d * BM + BM, 0:BM]))
        potential = dot_three(split_two(left), esp)
        rows = slice(d * BD, d * BD + BD)
        core = jnp.concatenate([first_ref[rows, :], second_ref[rows, 0:64]], axis=1)
        total = core + potential
        core_out[d] = 0.5 * (total + total.T)

    def live_count(d):
        n_first = jnp.clip(sizes_ref[0, d], 0, BM)
        n_second = jnp.clip(sizes_ref[1, d], 0, BM)
        return n_first, n_second, (n_first + n_second).astype(f32)

    def purify(source, singles):
        for d in range(LOCAL):
            n_first, n_second, count = live_count(d)
            live, diagonal = live_square(n_first, n_second)
            masked = jnp.where(live, source[d], 0.0)
            on_diagonal = jnp.logical_and(live, diagonal)
            chemical = jnp.sum(jnp.where(diagonal, masked, 0.0)) / count
            shifted = masked - jnp.where(on_diagonal, chemical, 0.0)
            radius = jnp.max(jnp.sum(jnp.abs(shifted), axis=0, keepdims=True))
            work[d] = shifted * (-0.5 / (radius + epsilon))

        def single(_, carry):
            for d in range(LOCAL):
                high = work[d].astype(bf16)
                work_h[d] = high
                square_h[d] = dot(high, high).astype(bf16)
            for d in range(LOCAL):
                work[d] = 1.5 * work[d] - 2.0 * dot(square_h[d], work_h[d])
            return carry

        def triple(_, carry):
            for d in range(LOCAL):
                high, low = split_two(work[d])
                work_h[d] = high
                work_l[d] = low
                squared = dot_three((high, low), (high, low))
                square_h[d], square_l[d] = split_two(squared)
            for d in range(LOCAL):
                cubed = dot_three((square_h[d], square_l[d]), (work_h[d], work_l[d]))
                work[d] = 1.5 * work[d] - 2.0 * cubed
            return carry

        if singles > 0:
            lax.fori_loop(0, singles, single, 0)
        if singles < PURIFY:
            lax.fori_loop(singles, PURIFY, triple, 0)

    def density_of(d):
        n_first, n_second, count = live_count(d)
        live, diagonal = live_square(n_first, n_second)
        return work[d] + jnp.where(jnp.logical_and(live, diagonal), 0.5, 0.0), diagonal, count

    purify(core_out, SINGLE[0])
    for d in range(LOCAL):
        density, diagonal, _ = density_of(d)
        diagonals[d : d + 1, :] = jnp.sum(jnp.where(diagonal, density, 0.0), axis=0, keepdims=True)
    coulomb = jnp.dot(diagonals[...], repulsion, precision=highest, preferred_element_type=f32)
    for d in range(LOCAL):
        density, diagonal, _ = density_of(d)
        fock[d] = (
            core_out[d]
            + jnp.where(diagonal, coulomb[d : d + 1, :], 0.0)
            - 0.5 * (repulsion * density)
        )
    purify(fock, SINGLE[1])
    energy = jnp.zeros((1, BD), f32)
    for d in range(LOCAL):
        density, _, count = density_of(d)
        density_out[d] = density
        terms = jnp.sum(density * (core_out[d] + fock[d]), axis=0, keepdims=True)
        energy = energy + terms * (0.5 / count)
    energy_out[...] = jnp.full((8, 128), jnp.sum(energy), f32)


def solve(segment, sizes, mine, theirs, first, second, esp_map, repulsion):
    vmem = pl.BlockSpec(memory_space=pltpu.VMEM)
    smem = pl.BlockSpec(memory_space=pltpu.SMEM)
    square = (LOCAL, BD, BD)
    return pl.pallas_call(
        solve_kernel,
        name="solve",
        in_specs=[smem, smem] + [pl.BlockSpec(memory_space=pltpu.HBM)] * 6,
        out_specs=[vmem] * 2,
        out_shape=[
            jax.ShapeDtypeStruct((2,) + square, f32),
            jax.ShapeDtypeStruct((8, 128), f32),
        ],
        scratch_shapes=[
            pltpu.VMEM((LOCAL, HALF), f32),
            pltpu.VMEM((LOCAL, HALF), f32),
            pltpu.VMEM((LOCAL * BD, 128), f32),
            pltpu.VMEM((LOCAL * BD, 128), f32),
            pltpu.VMEM((BM, BD), f32),
            pltpu.VMEM((BD, BD), f32),
            pltpu.SemaphoreType.DMA((6,)),
            pltpu.VMEM((LOCAL * FPITCH, 128), f32),
            pltpu.VMEM((LOCAL * BM, 128), f32),
            pltpu.VMEM(square, f32),
            pltpu.VMEM(square, f32),
            pltpu.VMEM(square, bf16),
            pltpu.VMEM(square, bf16),
            pltpu.VMEM(square, bf16),
            pltpu.VMEM(square, bf16),
            pltpu.VMEM((LOCAL, BD), f32),
        ],
        cost_estimate=pl.CostEstimate(
            flops=11000000000, bytes_accessed=6000000, transcendentals=0
        ),
    )(segment, sizes, mine, theirs, first, second, esp_map, repulsion)


def esp_weights(first_ids, second_ids, centers, labels):
    middle = 0.5 * (centers[:, first_ids] + centers[:, second_ids])
    nearby = centers[:, labels]
    distance = jnp.zeros((first_ids.shape[0], labels.shape[0]), f32)
    for axis_pos in range(3):
        axis_gap = middle[axis_pos][:, None] - nearby[axis_pos][None, :]
        distance = distance + axis_gap * axis_gap
    weights = 1.0 / jnp.sqrt(distance + 1.0)
    excluded = (labels[None, :] == first_ids[:, None]) | (labels[None, :] == second_ids[:, None])
    return jnp.where(excluded, 0.0, weights)


def after(values, anchor):
    return lax.optimization_barrier((values, anchor))[0]


def on_device(
    monomer_density, monomer_centers, dimer_pairs, basis_sizes, dimer_core, esp_map, repulsion
):
    chip = lax.axis_index(GRP)
    segment = lax.axis_index("segment")

    own = lax.dynamic_slice_in_dim(monomer_density, segment * HALF, HALF, 1)
    gathered = jnp.concatenate([own] + shifts(phase_shift, own, 0), axis=0)
    blocks = [gathered] + shifts(phase_shift, gathered, 1)

    pair_ids, centers = after((dimer_pairs, monomer_centers), gathered)
    strides = [jnp.where(segment == 0, STRIDES[0][p], STRIDES[1][p]) for p in range(3)]
    places = [(chip // strides[p]) % 4 for p in range(3)]

    def moved(chips, phase, step):
        return chips + ((places[phase] + step + 4) % 4 - places[phase]) * strides[phase]

    steps = jnp.arange(4, dtype=jnp.int32)
    targets = moved(chip, 2, steps)
    rows = (jnp.arange(16, dtype=jnp.int32) + 8 * segment) % 16
    dimers = (targets[:, None] * 16 + rows[None, :]).reshape(64)
    sources = moved(moved(chip, 0, -steps)[None, :], 1, -steps[:, None])
    labels = (sources[:, :, None] * 8 + jnp.arange(8, dtype=jnp.int32)).reshape(128)
    pairs = pair_ids[:, dimers]
    weights = esp_weights(pairs[0], pairs[1], centers, labels).astype(bf16)
    parts = partial_fields(weights, blocks)

    segment_array = segment.reshape(1).astype(jnp.int32)
    core_rows, sizes_all, esp, rep = after((dimer_core, basis_sizes, esp_map, repulsion), parts[0])
    first, second = unflatten(segment_array, core_rows)
    sizes = sizes_all[pairs.reshape(2, 4, 16)[:, 0, 0:8]]
    square_repulsion = rep.reshape(BD, BD)

    r0 = parts[0]
    r1, r2, r3 = shifts(lambda step: phase_shift(parts[step], 2, step))
    r1, r2, r3, first, second, sizes, esp, square_repulsion = lax.optimization_barrier(
        (r1, r2, r3, first, second, sizes, esp, square_repulsion)
    )
    own_sum, other_sum = [(r0[h] + r1[h]) + (r2[h] + r3[h]) for h in (slice(0, 8), slice(8, 16))]
    theirs = swap_cores(other_sum)
    stack, energy = solve(
        segment_array, sizes, own_sum, theirs, first, second, esp, square_repulsion
    )

    for axis in GRP:
        one, two, three = shifts(axis_shift, energy, axis)
        energy = (energy + two) + (one + three)
    energy = energy + swap_cores(energy)
    window_energy = energy[0, 0] / 1024.0

    sent = flatten(jnp.stack([1 - segment, 0 * segment]).astype(jnp.int32), stack, LOCAL)
    arrived = swap_cores(sent)
    kept = flatten(jnp.stack([segment, segment]).astype(jnp.int32), stack, 2 * LOCAL)
    combined = lax.dynamic_update_slice_in_dim(kept, arrived, (1 - segment) * LOCAL, 0)
    return (combined[None], window_energy)


def solution(mesh):
    split = Mesh(
        mesh.devices.reshape(mesh.shape["segment"], 4, 4, 4), ("segment", "grp_0", "grp_1", "grp_2")
    )
    return jax.shard_map(
        on_device,
        mesh=split,
        in_specs=(P(GRP, None), P(), P(), P(), P(GRP, None), P(), P()),
        out_specs=(P("segment", GRP, None), P()),
        check_vma=False,
    )
```

```python
import jax
import jax.numpy as jnp
from jax import lax
from jax.experimental import pallas as pl
from jax.experimental.pallas import tpu as pltpu
from jax.sharding import Mesh
from jax.sharding import PartitionSpec as P


PURIFY = 8
MIB = 1024 * 1024
SINGLE = (8, 4)
GRP = ("grp_0", "grp_1", "grp_2")
ALL = ("segment", "grp_0", "grp_1", "grp_2")
STRIDES = ((1, 4, 16), (4, 16, 1))

BM = 96
BD = 192
FLAT = BD * BD
TILES = FLAT // 128
HALF = BM * BM // 2
LOCAL = 8
PITCH = 292
FPITCH = 73
epsilon = 1e-06
f32 = jnp.float32
bf16 = jnp.bfloat16


def phase_shift(value, phase, step):
    pairs = []
    for core in range(2):
        stride = STRIDES[core][phase]
        for chip in range(64):
            place = (chip // stride) % 4
            target = chip + (((place + step) % 4) - place) * stride
            pairs.append((core * 64 + chip, core * 64 + target))
    return lax.ppermute(value, ALL, pairs)


def shifts(shift, *args):
    arrived = []
    for step in (1, 2, 3):
        arrived.append(shift(*args, step))
    return arrived


def axis_shift(value, axis, step):
    return lax.ppermute(value, axis, [(i, (i + step) % 4) for i in range(4)])


def swap_cores(value):
    return lax.ppermute(value, "segment", [(0, 1), (1, 0)])


def split_two(value):
    high = value.astype(bf16)
    low = (value - high.astype(f32)).astype(bf16)
    return high, low


def dot(left, right):
    return jnp.dot(left, right, preferred_element_type=f32)


def dot_three(left, right):
    (lh, ll), (rh, rl) = left, right
    return dot(lh, rh) + (dot(ll, rh) + dot(lh, rl))


def lane_index(rows):
    return lax.broadcasted_iota(jnp.int32, (rows, 128), 1)


def unflatten_kernel(segment_ref, core_ref, esp_ref, first_ref, second_ref, left_ref, flat):
    half = BM // 2
    own = pl.multiple_of(half * segment_ref[0], 8)
    other = pl.multiple_of(half - own, 8)
    left_ref[0:half, :] = esp_ref[pl.ds(own, half), :]
    left_ref[half:BM, :] = esp_ref[pl.ds(other, half), :]
    for tile in range(TILES):
        flat[pl.ds(tile, LOCAL, stride=PITCH), :] = core_ref[:, tile * 128 : tile * 128 + 128]
    low_half = lane_index(BM) < 64
    for d in range(LOCAL):
        a = flat[pl.ds(d * PITCH, BM, stride=3), :]
        b = flat[pl.ds(d * PITCH + 1, BM, stride=3), :]
        c = flat[pl.ds(d * PITCH + 2, BM, stride=3), :]
        b_rolled = pltpu.roll(b, 64, 1)
        c_rolled = pltpu.roll(c, 64, 1)
        first_ref[pl.ds(d * BD, BM, stride=2), :] = a
        second_ref[pl.ds(d * BD, BM, stride=2), :] = b
        first_ref[pl.ds(d * BD + 1, BM, stride=2), :] = jnp.where(low_half, b_rolled, c_rolled)
        second_ref[pl.ds(d * BD + 1, BM, stride=2), :] = c_rolled


def unflatten(segment, core, esp_map):
    return pl.pallas_call(
        unflatten_kernel,
        name="unflatten",
        grid_spec=pltpu.PrefetchScalarGridSpec(
            num_scalar_prefetch=1,
            grid=(1,),
            in_specs=[
                pl.BlockSpec((LOCAL, FLAT), lambda i, s: (s[0], 0)),
                pl.BlockSpec((BM, BD), lambda i, s: (0, 0)),
            ],
            out_specs=[pl.BlockSpec((LOCAL * BD, 128), lambda i, s: (0, 0))] * 2
            + [pl.BlockSpec((BM, BD), lambda i, s: (0, 0))],
            scratch_shapes=[pltpu.VMEM((LOCAL * PITCH, 128), f32)],
        ),
        out_shape=[jax.ShapeDtypeStruct((LOCAL * BD, 128), f32)] * 2
        + [jax.ShapeDtypeStruct((BM, BD), f32)],
        cost_estimate=pl.CostEstimate(flops=20000000, bytes_accessed=3000000, transcendentals=0),
    )(segment, core, esp_map)


def flatten_kernel(place_ref, square_ref, out_ref, first, second, flat):
    low_half = lane_index(BM) < 64
    for d in range(LOCAL):
        first[...] = square_ref[0, d, :, 0:128]
        second[:, 0:64] = square_ref[0, d, :, 128:192]
        even_a = first[pl.ds(0, BM, stride=2), :]
        even_b = second[pl.ds(0, BM, stride=2), :]
        odd_a = pltpu.roll(first[pl.ds(1, BM, stride=2), :], 64, 1)
        odd_b = pltpu.roll(second[pl.ds(1, BM, stride=2), :], 64, 1)
        flat[pl.ds(d * PITCH, BM, stride=3), :] = even_a
        flat[pl.ds(d * PITCH + 1, BM, stride=3), :] = jnp.where(low_half, even_b, odd_a)
        flat[pl.ds(d * PITCH + 2, BM, stride=3), :] = jnp.where(low_half, odd_a, odd_b)
    for tile in range(TILES):
        out_ref[:, tile * 128 : tile * 128 + 128] = flat[pl.ds(tile, LOCAL, stride=PITCH), :]


def flatten(place, stack, rows):
    return pl.pallas_call(
        flatten_kernel,
        name="flatten",
        grid_spec=pltpu.PrefetchScalarGridSpec(
            num_scalar_prefetch=1,
            grid=(1,),
            in_specs=[pl.BlockSpec((1, LOCAL, BD, BD), lambda i, p: (p[0], 0, 0, 0))],
            out_specs=pl.BlockSpec((LOCAL, FLAT), lambda i, p: (p[1], 0)),
            scratch_shapes=[
                pltpu.VMEM((BD, 128), f32),
                pltpu.VMEM((BD, 128), f32),
                pltpu.VMEM((LOCAL * PITCH, 128), f32),
            ],
        ),
        out_shape=pltpu.HBM((rows, FLAT), f32),
        cost_estimate=pl.CostEstimate(flops=20000000, bytes_accessed=3000000, transcendentals=0),
    )(place, stack)


def partial_kernel(weight_ref, b0, b1, b2, b3, o0, o1, o2, o3):
    for start in range(0, HALF, 512):
        columns = slice(start, start + 512)
        rows = jnp.concatenate([b[:, columns] for b in (b0, b1, b2, b3)], axis=0)
        total = dot(weight_ref[...], rows)
        for k, out in enumerate((o0, o1, o2, o3)):
            out[:, columns] = total[16 * k : 16 * k + 16]


def partial_fields(weights, blocks):
    return pl.pallas_call(
        partial_kernel,
        name="partial_fields",
        out_shape=[pltpu.HBM((16, HALF), f32)] * 4,
        compiler_params=pltpu.CompilerParams(vmem_limit_bytes=12 * MIB),
        cost_estimate=pl.CostEstimate(flops=80000000, bytes_accessed=2400000, transcendentals=0),
    )(weights, *blocks)


def solve_kernel(
    sizes_any, mine_any, theirs_any, first_any, second_any, esp_any, left_any, rep_any,
    stack, energy_out,
    sizes_ref, mine_ref, theirs_ref, first_ref, second_ref, esp_ref, left_ref, rep_ref, arrivals,
    fock, density, departures, flat, field, eye, masked, offset, work, work_h, work_l, square_h, square_l,
    alive, diagonal, others, scale, shift, occupied, extra,
):
    places = (
        (sizes_any, sizes_ref), (mine_any, mine_ref), (theirs_any, theirs_ref), (esp_any, esp_ref),
        (left_any, left_ref), (rep_any, rep_ref),
        (first_any, first_ref), (second_any, second_ref),
    )
    copies = [
        pltpu.make_async_copy(source, target, arrivals.at[i])
        for i, (source, target) in enumerate(places)
    ]
    for copy in copies:
        copy.start()

    row = lax.broadcasted_iota(jnp.int32, (BM, BD), 0)
    eye[...] = jnp.where(
        lax.broadcasted_iota(jnp.int32, (128, 128), 0) == lax.broadcasted_iota(jnp.int32, (128, 128), 1),
        1.0,
        0.0,
    )
    copies[0].wait()
    limits = [jnp.broadcast_to(sizes_ref[:, k : k + 1], (LOCAL, BD)) for k in (0, 1)]
    position = lax.broadcasted_iota(jnp.int32, (LOCAL, BD), 1)
    limit = jnp.where(position < BM, limits[0], limits[1] + BM)
    live = jnp.where(position < limit, 1.0, 0.0)
    alive[...] = live
    count = jnp.sum(live, axis=1, keepdims=True)

    for copy in copies[1:6]:
        copy.wait()
    for tile in range(36):
        columns = slice(tile * 128, tile * 128 + 128)
        flat[pl.ds(tile, LOCAL, stride=FPITCH), :] = mine_ref[:, columns]
        flat[pl.ds(36 + tile, LOCAL, stride=FPITCH), :] = theirs_ref[:, columns]
    lane = lane_index(24)
    for d in range(LOCAL):
        a = flat[pl.ds(d * FPITCH, 24, stride=3), :]
        b = flat[pl.ds(d * FPITCH + 1, 24, stride=3), :]
        c = flat[pl.ds(d * FPITCH + 2, 24, stride=3), :]
        base = d * BM
        field[pl.ds(base, 24, stride=4), :] = a
        field[pl.ds(base + 1, 24, stride=4), :] = jnp.where(
            lane < 32, pltpu.roll(a, 32, 1), pltpu.roll(b, 32, 1)
        )
        field[pl.ds(base + 2, 24, stride=4), :] = jnp.where(
            lane < 64, pltpu.roll(b, 64, 1), pltpu.roll(c, 64, 1)
        )
        field[pl.ds(base + 3, 24, stride=4), :] = pltpu.roll(c, 96, 1)

    esp = split_two(esp_ref[...])
    esp_t = split_two(left_ref[...].T)
    repulsion = 0.5 * (rep_ref[...] + rep_ref[...].T)
    half_repulsion = 0.5 * repulsion
    right = split_two(dot_three(split_two(field[...][:, 0:BM]), esp))

    def blocks(value):
        return value[0:128, 0:128], value[128:BD, 128:BD]

    def eyes():
        return eye[...], eye[0:64, 0:64]

    def diagonal_of(value):
        first_part, second_part = (
            jnp.sum(b * e, axis=0, keepdims=True) for b, e in zip(blocks(value), eyes())
        )
        return jnp.concatenate([first_part, second_part], axis=1)

    def with_diagonal(value, vector):
        (a, b), (eye_a, eye_b) = blocks(value), eyes()
        a = a + eye_a * vector[:, 0:128]
        b = b + eye_b * vector[:, 128:BD]
        return jnp.concatenate(
            [
                jnp.concatenate([a, value[0:128, 128:BD]], axis=1),
                jnp.concatenate([value[128:BD, 0:128], b], axis=1),
            ],
            axis=0,
        )

    def columns_of(value, d):
        (a, b), (eye_a, eye_b) = blocks(value), eyes()
        on_a, on_b = a * eye_a, b * eye_b
        diagonal[d : d + 1, 0:128] = jnp.sum(on_a, axis=0, keepdims=True)
        diagonal[d : d + 1, 128:BD] = jnp.sum(on_b, axis=0, keepdims=True)

        def total(part):
            return jnp.sum(jnp.abs(part), axis=0, keepdims=True)

        others[d : d + 1, 0:128] = total(a - on_a) + total(value[128:BD, 0:128])
        others[d : d + 1, 128:BD] = total(b - on_b) + total(value[0:128, 128:BD])

    copies[6].wait()
    copies[7].wait()
    for d in range(LOCAL):
        rows = slice(d * BM, d * BM + BM)
        potential = dot_three(esp_t, (right[0][rows], right[1][rows]))
        rows = slice(d * BD, d * BD + BD)
        core = jnp.concatenate([first_ref[rows, :], second_ref[rows, 0:64]], axis=1)
        total = core + potential
        total = 0.5 * (total + total.T)
        fock[d] = total
        total = total * alive[d : d + 1, :]
        total = jnp.concatenate(
            [
                jnp.where(row < limits[0][d : d + 1, :], total[0:BM], 0.0),
                jnp.where(row < limits[1][d : d + 1, :], total[BM:BD], 0.0),
            ],
            axis=0,
        )
        masked[d] = total
        columns_of(total, d)

    leaving = [pltpu.make_async_copy(fock, stack.at[0], departures.at[LOCAL])]
    leaving[0].start()

    def start(source, added):
        on_diagonal = diagonal[...] + added
        chemical = jnp.sum(on_diagonal, axis=1, keepdims=True) / count
        lowered = chemical * live
        sums = others[...] + jnp.abs(on_diagonal - lowered)
        radius = jnp.max(sums, axis=1, keepdims=True)
        scale[...] = jnp.broadcast_to(-0.5 / (radius + epsilon), (LOCAL, BD))
        shift[...] = added - lowered
        for d in range(LOCAL):
            work[d] = with_diagonal(source[d], shift[d : d + 1, :]) * scale[d : d + 1, :]

    def single(_, carry):
        for d in range(LOCAL):
            high = work[d].astype(bf16)
            work_h[d] = high
            square_h[d] = dot(high, high).astype(bf16)
        for d in range(LOCAL):
            work[d] = 1.5 * work[d] - 2.0 * dot(square_h[d], work_h[d])
        return carry

    def triple(_, carry):
        for d in range(LOCAL):
            high, low = split_two(work[d])
            work_h[d] = high
            work_l[d] = low
            squared = dot_three((high, low), (high, low))
            square_h[d], square_l[d] = split_two(squared)
        for d in range(LOCAL):
            cubed = dot_three((square_h[d], square_l[d]), (work_h[d], work_l[d]))
            work[d] = 1.5 * work[d] - 2.0 * cubed
        return carry

    def purify(singles):
        if singles > 0:
            lax.fori_loop(0, singles, single, 0)
        if singles < PURIFY:
            lax.fori_loop(singles, PURIFY, triple, 0)

    start(masked, jnp.zeros((LOCAL, BD), f32))
    purify(SINGLE[0])
    for d in range(LOCAL):
        occupied[d : d + 1, :] = diagonal_of(work[d])
    coulomb = dot_three(split_two(occupied[...] + 0.5 * live), split_two(repulsion))
    own_repulsion = diagonal_of(half_repulsion)
    extra[...] = live * (coulomb - 0.5 * own_repulsion)
    for d in range(LOCAL):
        changed = masked[d] - half_repulsion * work[d]
        offset[d] = changed
        columns_of(changed, d)
    start(offset, extra[...])
    purify(SINGLE[1])
    for d in range(LOCAL):
        solved = with_diagonal(work[d], 0.5 * alive[d : d + 1, :])
        density[d] = solved
        leaving.append(pltpu.make_async_copy(density.at[d], stack.at[1, d], departures.at[d]))
        leaving[-1].start()
        both = with_diagonal(masked[d] + offset[d], extra[d : d + 1, :])
        diagonal[d : d + 1, :] = jnp.sum(solved * both, axis=0, keepdims=True)
    energy = jnp.sum(diagonal[...], axis=1, keepdims=True) * (0.5 / count)
    energy_out[...] = jnp.broadcast_to(jnp.sum(energy, axis=0, keepdims=True), (8, 128))
    for copy in leaving:
        copy.wait()


def solve(sizes, mine, theirs, first, second, esp_map, esp_left, repulsion):
    vmem = pl.BlockSpec(memory_space=pltpu.VMEM)
    square = (LOCAL, BD, BD)
    return pl.pallas_call(
        solve_kernel,
        name="solve",
        in_specs=[pl.BlockSpec(memory_space=pltpu.HBM)] * 8,
        out_specs=[pl.BlockSpec(memory_space=pltpu.HBM), vmem],
        out_shape=[
            jax.ShapeDtypeStruct((2,) + square, f32),
            jax.ShapeDtypeStruct((8, 128), f32),
        ],
        scratch_shapes=[
            pltpu.VMEM((LOCAL, 2), jnp.int32),
            pltpu.VMEM((LOCAL, HALF), f32),
            pltpu.VMEM((LOCAL, HALF), f32),
            pltpu.VMEM((LOCAL * BD, 128), f32),
            pltpu.VMEM((LOCAL * BD, 128), f32),
            pltpu.VMEM((BM, BD), f32),
            pltpu.VMEM((BM, BD), f32),
            pltpu.VMEM((BD, BD), f32),
            pltpu.SemaphoreType.DMA((8,)),
            pltpu.VMEM(square, f32),
            pltpu.VMEM(square, f32),
            pltpu.SemaphoreType.DMA((LOCAL + 1,)),
            pltpu.VMEM((LOCAL * FPITCH, 128), f32),
            pltpu.VMEM((LOCAL * BM, 128), f32),
            pltpu.VMEM((128, 128), f32),
            pltpu.VMEM(square, f32),
            pltpu.VMEM(square, f32),
            pltpu.VMEM(square, f32),
            pltpu.VMEM(square, bf16),
            pltpu.VMEM(square, bf16),
            pltpu.VMEM(square, bf16),
            pltpu.VMEM(square, bf16),
        ]
        + [pltpu.VMEM((LOCAL, BD), f32)] * 7,
        cost_estimate=pl.CostEstimate(
            flops=11000000000, bytes_accessed=6000000, transcendentals=0
        ),
    )(sizes, mine, theirs, first, second, esp_map, esp_left, repulsion)


def esp_weights(first_ids, second_ids, centers, labels):
    middle = 0.5 * (centers[:, first_ids] + centers[:, second_ids])
    nearby = centers[:, labels]
    distance = jnp.zeros((first_ids.shape[0], labels.shape[0]), f32)
    for axis_pos in range(3):
        axis_gap = middle[axis_pos][:, None] - nearby[axis_pos][None, :]
        distance = distance + axis_gap * axis_gap
    weights = 1.0 / jnp.sqrt(distance + 1.0)
    excluded = (labels[None, :] == first_ids[:, None]) | (labels[None, :] == second_ids[:, None])
    return jnp.where(excluded, 0.0, weights)


def after(values, anchor):
    return lax.optimization_barrier((values, anchor))[0]


def on_device(
    monomer_density, monomer_centers, dimer_pairs, basis_sizes, dimer_core, esp_map, repulsion
):
    chip = lax.axis_index(GRP)
    segment = lax.axis_index("segment")

    own = lax.dynamic_slice_in_dim(monomer_density, segment * HALF, HALF, 1)
    gathered = jnp.concatenate([own] + shifts(phase_shift, own, 0), axis=0)
    blocks = [gathered] + shifts(phase_shift, gathered, 1)

    pair_ids, centers = after((dimer_pairs, monomer_centers), gathered)
    strides = [jnp.where(segment == 0, STRIDES[0][p], STRIDES[1][p]) for p in range(3)]
    places = [(chip // strides[p]) % 4 for p in range(3)]

    def moved(chips, phase, step):
        return chips + ((places[phase] + step + 4) % 4 - places[phase]) * strides[phase]

    steps = jnp.arange(4, dtype=jnp.int32)
    targets = moved(chip, 2, steps)
    rows = (jnp.arange(16, dtype=jnp.int32) + 8 * segment) % 16
    dimers = (targets[:, None] * 16 + rows[None, :]).reshape(64)
    sources = moved(moved(chip, 0, -steps)[None, :], 1, -steps[:, None])
    labels = (sources[:, :, None] * 8 + jnp.arange(8, dtype=jnp.int32)).reshape(128)
    pairs = pair_ids[:, dimers]
    weights = esp_weights(pairs[0], pairs[1], centers, labels).astype(bf16)
    parts = partial_fields(weights, blocks)

    segment_array = segment.reshape(1).astype(jnp.int32)
    core_rows, sizes_all, esp, rep = after((dimer_core, basis_sizes, esp_map, repulsion), parts[0])
    first, second, left = unflatten(segment_array, core_rows, esp)
    sizes = jnp.clip(sizes_all[pairs.reshape(2, 4, 16)[:, 0, 0:8]], 0, BM).T
    square_repulsion = rep.reshape(BD, BD)

    r0 = parts[0]
    r1, r2, r3 = shifts(lambda step: phase_shift(parts[step], 2, step))
    r1, r2, r3, first, second, sizes, esp, left, square_repulsion = lax.optimization_barrier(
        (r1, r2, r3, first, second, sizes, esp, left, square_repulsion)
    )
    own_sum, other_sum = [(r0[h] + r1[h]) + (r2[h] + r3[h]) for h in (slice(0, 8), slice(8, 16))]
    theirs = swap_cores(other_sum)
    stack, energy = solve(
        sizes, own_sum, theirs, first, second, esp, left, square_repulsion
    )

    for axis in GRP:
        one, two, three = shifts(axis_shift, energy, axis)
        energy = (energy + two) + (one + three)
    energy = energy + swap_cores(energy)
    window_energy = energy[0, 0] / 1024.0

    sent = flatten(jnp.stack([1 - segment, 0 * segment]).astype(jnp.int32), stack, LOCAL)
    arrived = swap_cores(sent)
    kept = flatten(jnp.stack([segment, segment]).astype(jnp.int32), stack, 2 * LOCAL)
    combined = lax.dynamic_update_slice_in_dim(kept, arrived, (1 - segment) * LOCAL, 0)
    return (combined[None], window_energy)


def solution(mesh):
    split = Mesh(
        mesh.devices.reshape(mesh.shape["segment"], 4, 4, 4), ("segment", "grp_0", "grp_1", "grp_2")
    )
    return jax.shard_map(
        on_device,
        mesh=split,
        in_specs=(P(GRP, None), P(), P(), P(), P(GRP, None), P(), P()),
        out_specs=(P("segment", GRP, None), P()),
        check_vma=False,
    )
```

```python
import jax
import jax.numpy as jnp
from jax import lax
from jax.experimental import pallas as pl
from jax.experimental.pallas import tpu as pltpu
from jax.sharding import Mesh
from jax.sharding import PartitionSpec as P


PURIFY = 8
MIB = 1024 * 1024
SINGLE = (8, 4)
GRP = ("grp_0", "grp_1", "grp_2")
ALL = ("segment", "grp_0", "grp_1", "grp_2")
STRIDES = ((1, 4, 16), (4, 16, 1))

BM = 96
BD = 192
FLAT = BD * BD
TILES = FLAT // 128
HALF = BM * BM // 2
LOCAL = 8
PITCH = 292
FPITCH = 73
epsilon = 1e-06
f32 = jnp.float32
bf16 = jnp.bfloat16


def phase_shift(value, phase, step):
    pairs = []
    for core in range(2):
        stride = STRIDES[core][phase]
        for chip in range(64):
            place = (chip // stride) % 4
            target = chip + (((place + step) % 4) - place) * stride
            pairs.append((core * 64 + chip, core * 64 + target))
    return lax.ppermute(value, ALL, pairs)


def shifts(shift, *args):
    arrived = []
    for step in (1, 2, 3):
        arrived.append(shift(*args, step))
    return arrived


def axis_shift(value, axis, step):
    return lax.ppermute(value, axis, [(i, (i + step) % 4) for i in range(4)])


def swap_cores(value):
    return lax.ppermute(value, "segment", [(0, 1), (1, 0)])


def split_two(value):
    high = value.astype(bf16)
    low = (value - high.astype(f32)).astype(bf16)
    return high, low


def dot(left, right):
    return jnp.dot(left, right, preferred_element_type=f32)


def dot_three(left, right):
    (lh, ll), (rh, rl) = left, right
    return dot(lh, rh) + (dot(ll, rh) + dot(lh, rl))


def lane_index(rows):
    return lax.broadcasted_iota(jnp.int32, (rows, 128), 1)


def unflatten_kernel(segment_ref, core_ref, esp_ref, first_ref, second_ref, left_ref, flat):
    half = BM // 2
    own = pl.multiple_of(half * segment_ref[0], 8)
    other = pl.multiple_of(half - own, 8)
    left_ref[0:half, :] = esp_ref[pl.ds(own, half), :]
    left_ref[half:BM, :] = esp_ref[pl.ds(other, half), :]
    for tile in range(TILES):
        flat[pl.ds(tile, LOCAL, stride=PITCH), :] = core_ref[:, tile * 128 : tile * 128 + 128]
    low_half = lane_index(BM) < 64
    for d in range(LOCAL):
        a = flat[pl.ds(d * PITCH, BM, stride=3), :]
        b = flat[pl.ds(d * PITCH + 1, BM, stride=3), :]
        c = flat[pl.ds(d * PITCH + 2, BM, stride=3), :]
        b_rolled = pltpu.roll(b, 64, 1)
        c_rolled = pltpu.roll(c, 64, 1)
        first_ref[pl.ds(d * BD, BM, stride=2), :] = a
        second_ref[pl.ds(d * BD, BM, stride=2), :] = b
        first_ref[pl.ds(d * BD + 1, BM, stride=2), :] = jnp.where(low_half, b_rolled, c_rolled)
        second_ref[pl.ds(d * BD + 1, BM, stride=2), :] = c_rolled


def unflatten(segment, core, esp_map):
    return pl.pallas_call(
        unflatten_kernel,
        name="unflatten",
        grid_spec=pltpu.PrefetchScalarGridSpec(
            num_scalar_prefetch=1,
            grid=(1,),
            in_specs=[
                pl.BlockSpec((LOCAL, FLAT), lambda i, s: (s[0], 0)),
                pl.BlockSpec((BM, BD), lambda i, s: (0, 0)),
            ],
            out_specs=[pl.BlockSpec((LOCAL * BD, 128), lambda i, s: (0, 0))] * 2
            + [pl.BlockSpec((BM, BD), lambda i, s: (0, 0))],
            scratch_shapes=[pltpu.VMEM((LOCAL * PITCH, 128), f32)],
        ),
        out_shape=[jax.ShapeDtypeStruct((LOCAL * BD, 128), f32)] * 2
        + [jax.ShapeDtypeStruct((BM, BD), f32)],
        cost_estimate=pl.CostEstimate(flops=20000000, bytes_accessed=3000000, transcendentals=0),
    )(segment, core, esp_map)


def flatten_kernel(place_ref, square_ref, out_ref, first, second, flat):
    low_half = lane_index(BM) < 64
    for d in range(LOCAL):
        first[...] = square_ref[0, d, :, 0:128]
        second[:, 0:64] = square_ref[0, d, :, 128:192]
        even_a = first[pl.ds(0, BM, stride=2), :]
        even_b = second[pl.ds(0, BM, stride=2), :]
        odd_a = pltpu.roll(first[pl.ds(1, BM, stride=2), :], 64, 1)
        odd_b = pltpu.roll(second[pl.ds(1, BM, stride=2), :], 64, 1)
        flat[pl.ds(d * PITCH, BM, stride=3), :] = even_a
        flat[pl.ds(d * PITCH + 1, BM, stride=3), :] = jnp.where(low_half, even_b, odd_a)
        flat[pl.ds(d * PITCH + 2, BM, stride=3), :] = jnp.where(low_half, odd_a, odd_b)
    for tile in range(TILES):
        out_ref[:, tile * 128 : tile * 128 + 128] = flat[pl.ds(tile, LOCAL, stride=PITCH), :]


def flatten(place, stack, rows):
    return pl.pallas_call(
        flatten_kernel,
        name="flatten",
        grid_spec=pltpu.PrefetchScalarGridSpec(
            num_scalar_prefetch=1,
            grid=(1,),
            in_specs=[pl.BlockSpec((1, LOCAL, BD, BD), lambda i, p: (p[0], 0, 0, 0))],
            out_specs=pl.BlockSpec((LOCAL, FLAT), lambda i, p: (p[1], 0)),
            scratch_shapes=[
                pltpu.VMEM((BD, 128), f32),
                pltpu.VMEM((BD, 128), f32),
                pltpu.VMEM((LOCAL * PITCH, 128), f32),
            ],
        ),
        out_shape=pltpu.HBM((rows, FLAT), f32),
        cost_estimate=pl.CostEstimate(flops=20000000, bytes_accessed=3000000, transcendentals=0),
    )(place, stack)


def partial_kernel(weight_ref, b0, b1, b2, b3, o0, o1, o2, o3):
    for start in range(0, HALF, 512):
        columns = slice(start, start + 512)
        rows = jnp.concatenate([b[:, columns] for b in (b0, b1, b2, b3)], axis=0)
        total = dot(weight_ref[...], rows)
        for k, out in enumerate((o0, o1, o2, o3)):
            out[:, columns] = total[16 * k : 16 * k + 16]


def partial_fields(weights, blocks):
    return pl.pallas_call(
        partial_kernel,
        name="partial_fields",
        out_shape=[pltpu.HBM((16, HALF), f32)] * 4,
        compiler_params=pltpu.CompilerParams(vmem_limit_bytes=12 * MIB),
        cost_estimate=pl.CostEstimate(flops=80000000, bytes_accessed=2400000, transcendentals=0),
    )(weights, *blocks)


def solve_kernel(
    sizes_any, mine_any, theirs_any, first_any, second_any, esp_any, left_any, rep_any,
    stack, energy_out,
    sizes_ref, mine_ref, theirs_ref, first_ref, second_ref, esp_ref, left_ref, rep_ref, arrivals,
    fock, density, departures, flat, field, eye, masked, offset, work, work_h, work_l, square_h, square_l,
    alive, diagonal, others, scale, shift, occupied, extra,
):
    places = (
        (sizes_any, sizes_ref), (mine_any, mine_ref), (theirs_any, theirs_ref), (esp_any, esp_ref),
        (left_any, left_ref), (rep_any, rep_ref),
        (first_any, first_ref), (second_any, second_ref),
    )
    copies = [
        pltpu.make_async_copy(source, target, arrivals.at[i])
        for i, (source, target) in enumerate(places)
    ]
    for copy in copies:
        copy.start()

    row = lax.broadcasted_iota(jnp.int32, (BM, BD), 0)
    eye[...] = jnp.where(
        lax.broadcasted_iota(jnp.int32, (128, 128), 0) == lax.broadcasted_iota(jnp.int32, (128, 128), 1),
        1.0,
        0.0,
    )
    copies[0].wait()
    limits = [jnp.broadcast_to(sizes_ref[:, k : k + 1], (LOCAL, BD)) for k in (0, 1)]
    position = lax.broadcasted_iota(jnp.int32, (LOCAL, BD), 1)
    limit = jnp.where(position < BM, limits[0], limits[1] + BM)
    live = jnp.where(position < limit, 1.0, 0.0)
    alive[...] = live
    count = jnp.sum(live, axis=1, keepdims=True)

    for copy in copies[1:6]:
        copy.wait()
    for tile in range(36):
        columns = slice(tile * 128, tile * 128 + 128)
        flat[pl.ds(tile, LOCAL, stride=FPITCH), :] = mine_ref[:, columns]
        flat[pl.ds(36 + tile, LOCAL, stride=FPITCH), :] = theirs_ref[:, columns]
    lane = lane_index(24)
    for d in range(LOCAL):
        a = flat[pl.ds(d * FPITCH, 24, stride=3), :]
        b = flat[pl.ds(d * FPITCH + 1, 24, stride=3), :]
        c = flat[pl.ds(d * FPITCH + 2, 24, stride=3), :]
        base = d * BM
        field[pl.ds(base, 24, stride=4), :] = a
        field[pl.ds(base + 1, 24, stride=4), :] = jnp.where(
            lane < 32, pltpu.roll(a, 32, 1), pltpu.roll(b, 32, 1)
        )
        field[pl.ds(base + 2, 24, stride=4), :] = jnp.where(
            lane < 64, pltpu.roll(b, 64, 1), pltpu.roll(c, 64, 1)
        )
        field[pl.ds(base + 3, 24, stride=4), :] = pltpu.roll(c, 96, 1)

    esp = split_two(esp_ref[...])
    esp_t = split_two(left_ref[...].T)
    repulsion = 0.5 * (rep_ref[...] + rep_ref[...].T)
    half_repulsion = 0.5 * repulsion
    right = split_two(dot_three(split_two(field[...][:, 0:BM]), esp))

    def blocks(value):
        return value[0:128, 0:128], value[128:BD, 128:BD]

    def eyes():
        return eye[...], eye[0:64, 0:64]

    def diagonal_of(value):
        first_part, second_part = (
            jnp.sum(b * e, axis=0, keepdims=True) for b, e in zip(blocks(value), eyes())
        )
        return jnp.concatenate([first_part, second_part], axis=1)

    def with_diagonal(value, vector):
        (a, b), (eye_a, eye_b) = blocks(value), eyes()
        a = a + eye_a * vector[:, 0:128]
        b = b + eye_b * vector[:, 128:BD]
        return jnp.concatenate(
            [
                jnp.concatenate([a, value[0:128, 128:BD]], axis=1),
                jnp.concatenate([value[128:BD, 0:128], b], axis=1),
            ],
            axis=0,
        )

    def columns_of(value, d):
        (a, b), (eye_a, eye_b) = blocks(value), eyes()
        on_a, on_b = a * eye_a, b * eye_b
        diagonal[d : d + 1, 0:128] = jnp.sum(on_a, axis=0, keepdims=True)
        diagonal[d : d + 1, 128:BD] = jnp.sum(on_b, axis=0, keepdims=True)

        def total(part):
            return jnp.sum(jnp.abs(part), axis=0, keepdims=True)

        others[d : d + 1, 0:128] = total(a - on_a) + total(value[128:BD, 0:128])
        others[d : d + 1, 128:BD] = total(b - on_b) + total(value[0:128, 128:BD])

    copies[6].wait()
    copies[7].wait()
    for d in range(LOCAL):
        rows = slice(d * BM, d * BM + BM)
        potential = dot_three(esp_t, (right[0][rows], right[1][rows]))
        rows = slice(d * BD, d * BD + BD)
        core = jnp.concatenate([first_ref[rows, :], second_ref[rows, 0:64]], axis=1)
        total = core + potential
        total = 0.5 * (total + total.T)
        fock[d] = total
        total = total * alive[d : d + 1, :]
        total = jnp.concatenate(
            [
                jnp.where(row < limits[0][d : d + 1, :], total[0:BM], 0.0),
                jnp.where(row < limits[1][d : d + 1, :], total[BM:BD], 0.0),
            ],
            axis=0,
        )
        masked[d] = total
        columns_of(total, d)

    leaving = [pltpu.make_async_copy(fock, stack.at[0], departures.at[LOCAL])]
    leaving[0].start()

    def start(source, added):
        on_diagonal = diagonal[...] + added
        chemical = jnp.sum(on_diagonal, axis=1, keepdims=True) / count
        lowered = chemical * live
        sums = others[...] + jnp.abs(on_diagonal - lowered)
        radius = jnp.max(sums, axis=1, keepdims=True)
        scale[...] = jnp.broadcast_to(-0.5 / (radius + epsilon), (LOCAL, BD))
        shift[...] = added - lowered
        for d in range(LOCAL):
            work[d] = with_diagonal(source[d], shift[d : d + 1, :]) * scale[d : d + 1, :]

    def single(_, carry):
        for d in range(LOCAL):
            high = work[d].astype(bf16)
            work_h[d] = high
            square_h[d] = dot(high, high).astype(bf16)
        for d in range(LOCAL):
            work[d] = 1.5 * work[d] - 2.0 * dot(square_h[d], work_h[d])
        return carry

    def triple(_, carry):
        for d in range(LOCAL):
            high, low = split_two(work[d])
            work_h[d] = high
            work_l[d] = low
            squared = dot_three((high, low), (high, low))
            square_h[d], square_l[d] = split_two(squared)
        for d in range(LOCAL):
            cubed = dot_three((square_h[d], square_l[d]), (work_h[d], work_l[d]))
            work[d] = 1.5 * work[d] - 2.0 * cubed
        return carry

    def purify(singles):
        if singles > 0:
            lax.fori_loop(0, singles, single, 0)
        if singles < PURIFY:
            lax.fori_loop(singles, PURIFY, triple, 0, unroll=True)

    start(masked, jnp.zeros((LOCAL, BD), f32))
    purify(SINGLE[0])
    for d in range(LOCAL):
        occupied[d : d + 1, :] = diagonal_of(work[d])
    coulomb = dot_three(split_two(occupied[...] + 0.5 * live), split_two(repulsion))
    own_repulsion = diagonal_of(half_repulsion)
    extra[...] = live * (coulomb - 0.5 * own_repulsion)
    for d in range(LOCAL):
        changed = masked[d] - half_repulsion * work[d]
        offset[d] = changed
        columns_of(changed, d)
    start(offset, extra[...])
    purify(SINGLE[1])
    for d in range(LOCAL):
        solved = with_diagonal(work[d], 0.5 * alive[d : d + 1, :])
        density[d] = solved
        leaving.append(pltpu.make_async_copy(density.at[d], stack.at[1, d], departures.at[d]))
        leaving[-1].start()
        both = with_diagonal(masked[d] + offset[d], extra[d : d + 1, :])
        diagonal[d : d + 1, :] = jnp.sum(solved * both, axis=0, keepdims=True)
    energy = jnp.sum(diagonal[...], axis=1, keepdims=True) * (0.5 / (1024.0 * count))
    energy_out[...] = jnp.broadcast_to(jnp.sum(energy, axis=0, keepdims=True), (8, 128))
    for copy in leaving:
        copy.wait()


def solve(sizes, mine, theirs, first, second, esp_map, esp_left, repulsion):
    vmem = pl.BlockSpec(memory_space=pltpu.VMEM)
    square = (LOCAL, BD, BD)
    return pl.pallas_call(
        solve_kernel,
        name="solve",
        in_specs=[pl.BlockSpec(memory_space=pltpu.HBM)] * 8,
        out_specs=[pl.BlockSpec(memory_space=pltpu.HBM), vmem],
        out_shape=[
            jax.ShapeDtypeStruct((2,) + square, f32),
            jax.ShapeDtypeStruct((8, 128), f32),
        ],
        scratch_shapes=[
            pltpu.VMEM((LOCAL, 2), jnp.int32),
            pltpu.VMEM((LOCAL, HALF), f32),
            pltpu.VMEM((LOCAL, HALF), f32),
            pltpu.VMEM((LOCAL * BD, 128), f32),
            pltpu.VMEM((LOCAL * BD, 128), f32),
            pltpu.VMEM((BM, BD), f32),
            pltpu.VMEM((BM, BD), f32),
            pltpu.VMEM((BD, BD), f32),
            pltpu.SemaphoreType.DMA((8,)),
            pltpu.VMEM(square, f32),
            pltpu.VMEM(square, f32),
            pltpu.SemaphoreType.DMA((LOCAL + 1,)),
            pltpu.VMEM((LOCAL * FPITCH, 128), f32),
            pltpu.VMEM((LOCAL * BM, 128), f32),
            pltpu.VMEM((128, 128), f32),
            pltpu.VMEM(square, f32),
            pltpu.VMEM(square, f32),
            pltpu.VMEM(square, f32),
            pltpu.VMEM(square, bf16),
            pltpu.VMEM(square, bf16),
            pltpu.VMEM(square, bf16),
            pltpu.VMEM(square, bf16),
        ]
        + [pltpu.VMEM((LOCAL, BD), f32)] * 7,
        cost_estimate=pl.CostEstimate(
            flops=11000000000, bytes_accessed=6000000, transcendentals=0
        ),
    )(sizes, mine, theirs, first, second, esp_map, esp_left, repulsion)


def esp_weights(first_ids, second_ids, centers, labels):
    middle = 0.5 * (centers[:, first_ids] + centers[:, second_ids])
    nearby = centers[:, labels]
    distance = jnp.zeros((first_ids.shape[0], labels.shape[0]), f32)
    for axis_pos in range(3):
        axis_gap = middle[axis_pos][:, None] - nearby[axis_pos][None, :]
        distance = distance + axis_gap * axis_gap
    weights = 1.0 / jnp.sqrt(distance + 1.0)
    excluded = (labels[None, :] == first_ids[:, None]) | (labels[None, :] == second_ids[:, None])
    return jnp.where(excluded, 0.0, weights)


def after(values, anchor):
    return lax.optimization_barrier((values, anchor))[0]


def on_device(
    monomer_density, monomer_centers, dimer_pairs, basis_sizes, dimer_core, esp_map, repulsion
):
    chip = lax.axis_index(GRP)
    segment = lax.axis_index("segment")

    own = lax.dynamic_slice_in_dim(monomer_density, segment * HALF, HALF, 1)
    gathered = jnp.concatenate([own] + shifts(phase_shift, own, 0), axis=0)
    blocks = [gathered] + shifts(phase_shift, gathered, 1)

    pair_ids, centers = after((dimer_pairs, monomer_centers), gathered)
    strides = [jnp.where(segment == 0, STRIDES[0][p], STRIDES[1][p]) for p in range(3)]
    places = [(chip // strides[p]) % 4 for p in range(3)]

    def moved(chips, phase, step):
        return chips + ((places[phase] + step + 4) % 4 - places[phase]) * strides[phase]

    steps = jnp.arange(4, dtype=jnp.int32)
    targets = moved(chip, 2, steps)
    rows = (jnp.arange(16, dtype=jnp.int32) + 8 * segment) % 16
    dimers = (targets[:, None] * 16 + rows[None, :]).reshape(64)
    sources = moved(moved(chip, 0, -steps)[None, :], 1, -steps[:, None])
    labels = (sources[:, :, None] * 8 + jnp.arange(8, dtype=jnp.int32)).reshape(128)
    pairs = pair_ids[:, dimers]
    weights = esp_weights(pairs[0], pairs[1], centers, labels).astype(bf16)
    parts = partial_fields(weights, blocks)

    segment_array = segment.reshape(1).astype(jnp.int32)
    core_rows, sizes_all, esp, rep = after((dimer_core, basis_sizes, esp_map, repulsion), parts[0])
    first, second, left = unflatten(segment_array, core_rows, esp)
    sizes = jnp.clip(sizes_all[pairs.reshape(2, 4, 16)[:, 0, 0:8]], 0, BM).T
    square_repulsion = rep.reshape(BD, BD)

    r0 = parts[0]
    narrow = [part.astype(jnp.float16) for part in parts]
    r1, r2, r3 = shifts(lambda step: phase_shift(narrow[step], 2, step))
    r1, r2, r3, first, second, sizes, esp, left, square_repulsion = lax.optimization_barrier(
        (r1, r2, r3, first, second, sizes, esp, left, square_repulsion)
    )
    own_sum, other_sum = [
        (r0[h] + r1[h].astype(f32)) + (r2[h].astype(f32) + r3[h].astype(f32))
        for h in (slice(0, 8), slice(8, 16))
    ]
    theirs = swap_cores(other_sum)
    stack, energy = solve(
        sizes, own_sum, theirs, first, second, esp, left, square_repulsion
    )

    for axis in GRP:
        one, two, three = shifts(axis_shift, energy, axis)
        energy = (energy + two) + (one + three)
    energy = energy + swap_cores(energy)
    window_energy = energy[0, 0]

    sent = flatten(jnp.stack([1 - segment, 0 * segment]).astype(jnp.int32), stack, LOCAL)
    arrived = swap_cores(sent)
    kept = flatten(jnp.stack([segment, segment]).astype(jnp.int32), stack, 2 * LOCAL)
    combined = lax.dynamic_update_slice_in_dim(kept, arrived, (1 - segment) * LOCAL, 0)
    return (combined[None], window_energy)


def solution(mesh):
    split = Mesh(
        mesh.devices.reshape(mesh.shape["segment"], 4, 4, 4), ("segment", "grp_0", "grp_1", "grp_2")
    )
    return jax.shard_map(
        on_device,
        mesh=split,
        in_specs=(P(GRP, None), P(), P(), P(), P(GRP, None), P(), P()),
        out_specs=(P("segment", GRP, None), P()),
        check_vma=False,
    )
```

```python
import jax
import jax.numpy as jnp
from jax import lax
from jax.experimental import pallas as pl
from jax.experimental.pallas import tpu as pltpu
from jax.sharding import Mesh
from jax.sharding import PartitionSpec as P


PURIFY = 8
MIB = 1024 * 1024
SINGLE = (8, 5)
GRP = ("grp_0", "grp_1", "grp_2")
ALL = ("segment", "grp_0", "grp_1", "grp_2")
STRIDES = ((1, 4, 16), (4, 16, 1))

BM = 96
BD = 192
FLAT = BD * BD
TILES = FLAT // 128
HALF = BM * BM // 2
LOCAL = 8
PITCH = 292
FPITCH = 73
epsilon = 1e-06
f32 = jnp.float32
bf16 = jnp.bfloat16


def phase_shift(value, phase, step):
    pairs = []
    for core in range(2):
        stride = STRIDES[core][phase]
        for chip in range(64):
            place = (chip // stride) % 4
            target = chip + (((place + step) % 4) - place) * stride
            pairs.append((core * 64 + chip, core * 64 + target))
    return lax.ppermute(value, ALL, pairs)


def shifts(shift, *args):
    arrived = []
    for step in (1, 2, 3):
        arrived.append(shift(*args, step))
    return arrived


def axis_shift(value, axis, step):
    return lax.ppermute(value, axis, [(i, (i + step) % 4) for i in range(4)])


def swap_cores(value):
    return lax.ppermute(value, "segment", [(0, 1), (1, 0)])


def split_two(value):
    high = value.astype(bf16)
    low = (value - high.astype(f32)).astype(bf16)
    return high, low


def dot(left, right):
    return jnp.dot(left, right, preferred_element_type=f32)


def dot_three(left, right):
    (lh, ll), (rh, rl) = left, right
    return dot(lh, rh) + (dot(ll, rh) + dot(lh, rl))


def lane_index(rows):
    return lax.broadcasted_iota(jnp.int32, (rows, 128), 1)


def unflatten_kernel(segment_ref, core_ref, esp_ref, first_ref, second_ref, left_ref, flat):
    half = BM // 2
    own = pl.multiple_of(half * segment_ref[0], 8)
    other = pl.multiple_of(half - own, 8)
    left_ref[0:half, :] = esp_ref[pl.ds(own, half), :]
    left_ref[half:BM, :] = esp_ref[pl.ds(other, half), :]
    for tile in range(TILES):
        flat[pl.ds(tile, LOCAL, stride=PITCH), :] = core_ref[:, tile * 128 : tile * 128 + 128]
    low_half = lane_index(BM) < 64
    for d in range(LOCAL):
        a = flat[pl.ds(d * PITCH, BM, stride=3), :]
        b = flat[pl.ds(d * PITCH + 1, BM, stride=3), :]
        c = flat[pl.ds(d * PITCH + 2, BM, stride=3), :]
        b_rolled = pltpu.roll(b, 64, 1)
        c_rolled = pltpu.roll(c, 64, 1)
        first_ref[pl.ds(d * BD, BM, stride=2), :] = a
        second_ref[pl.ds(d * BD, BM, stride=2), :] = b
        first_ref[pl.ds(d * BD + 1, BM, stride=2), :] = jnp.where(low_half, b_rolled, c_rolled)
        second_ref[pl.ds(d * BD + 1, BM, stride=2), :] = c_rolled


def unflatten(segment, core, esp_map):
    return pl.pallas_call(
        unflatten_kernel,
        name="unflatten",
        grid_spec=pltpu.PrefetchScalarGridSpec(
            num_scalar_prefetch=1,
            grid=(1,),
            in_specs=[
                pl.BlockSpec((LOCAL, FLAT), lambda i, s: (s[0], 0)),
                pl.BlockSpec((BM, BD), lambda i, s: (0, 0)),
            ],
            out_specs=[pl.BlockSpec((LOCAL * BD, 128), lambda i, s: (0, 0))] * 2
            + [pl.BlockSpec((BM, BD), lambda i, s: (0, 0))],
            scratch_shapes=[pltpu.VMEM((LOCAL * PITCH, 128), f32)],
        ),
        out_shape=[jax.ShapeDtypeStruct((LOCAL * BD, 128), f32)] * 2
        + [jax.ShapeDtypeStruct((BM, BD), f32)],
        cost_estimate=pl.CostEstimate(flops=20000000, bytes_accessed=3000000, transcendentals=0),
    )(segment, core, esp_map)


def flatten_kernel(place_ref, square_ref, out_ref, first, second, flat):
    low_half = lane_index(BM) < 64
    for d in range(LOCAL):
        first[...] = square_ref[0, d, :, 0:128]
        second[:, 0:64] = square_ref[0, d, :, 128:192]
        even_a = first[pl.ds(0, BM, stride=2), :]
        even_b = second[pl.ds(0, BM, stride=2), :]
        odd_a = pltpu.roll(first[pl.ds(1, BM, stride=2), :], 64, 1)
        odd_b = pltpu.roll(second[pl.ds(1, BM, stride=2), :], 64, 1)
        flat[pl.ds(d * PITCH, BM, stride=3), :] = even_a
        flat[pl.ds(d * PITCH + 1, BM, stride=3), :] = jnp.where(low_half, even_b, odd_a)
        flat[pl.ds(d * PITCH + 2, BM, stride=3), :] = jnp.where(low_half, odd_a, odd_b)
    for tile in range(TILES):
        out_ref[:, tile * 128 : tile * 128 + 128] = flat[pl.ds(tile, LOCAL, stride=PITCH), :]


def flatten(place, stack, rows):
    return pl.pallas_call(
        flatten_kernel,
        name="flatten",
        grid_spec=pltpu.PrefetchScalarGridSpec(
            num_scalar_prefetch=1,
            grid=(1,),
            in_specs=[pl.BlockSpec((1, LOCAL, BD, BD), lambda i, p: (p[0], 0, 0, 0))],
            out_specs=pl.BlockSpec((LOCAL, FLAT), lambda i, p: (p[1], 0)),
            scratch_shapes=[
                pltpu.VMEM((BD, 128), f32),
                pltpu.VMEM((BD, 128), f32),
                pltpu.VMEM((LOCAL * PITCH, 128), f32),
            ],
        ),
        out_shape=pltpu.HBM((rows, FLAT), f32),
        cost_estimate=pl.CostEstimate(flops=20000000, bytes_accessed=3000000, transcendentals=0),
    )(place, stack)


def partial_kernel(weight_ref, b0, b1, b2, b3, o0, o1, o2, o3):
    for start in range(0, HALF, 512):
        columns = slice(start, start + 512)
        rows = jnp.concatenate([b[:, columns] for b in (b0, b1, b2, b3)], axis=0)
        total = dot(weight_ref[...], rows)
        for k, out in enumerate((o0, o1, o2, o3)):
            out[:, columns] = total[16 * k : 16 * k + 16]


def partial_fields(weights, blocks):
    return pl.pallas_call(
        partial_kernel,
        name="partial_fields",
        out_shape=[pltpu.HBM((16, HALF), f32)] + [pltpu.VMEM((16, HALF), f32)] * 3,
        compiler_params=pltpu.CompilerParams(vmem_limit_bytes=12 * MIB),
        cost_estimate=pl.CostEstimate(flops=80000000, bytes_accessed=2400000, transcendentals=0),
    )(weights, *blocks)


def solve_kernel(
    sizes_any, mine_any, theirs_any, first_any, second_any, esp_any, left_any, rep_any,
    stack, energy_out,
    sizes_ref, mine_ref, theirs_ref, first_ref, second_ref, esp_ref, left_ref, rep_ref, arrivals,
    fock, density, departures, flat, field, eye, masked, offset, work, work_h, work_l, square_h, square_l,
    alive, diagonal, others, scale, shift, occupied, extra,
):
    places = (
        (sizes_any, sizes_ref), (mine_any, mine_ref), (theirs_any, theirs_ref), (esp_any, esp_ref),
        (left_any, left_ref), (rep_any, rep_ref),
        (first_any, first_ref), (second_any, second_ref),
    )
    copies = [
        pltpu.make_async_copy(source, target, arrivals.at[i])
        for i, (source, target) in enumerate(places)
    ]
    for copy in copies:
        copy.start()

    row = lax.broadcasted_iota(jnp.int32, (BM, BD), 0)
    eye[...] = jnp.where(
        lax.broadcasted_iota(jnp.int32, (128, 128), 0) == lax.broadcasted_iota(jnp.int32, (128, 128), 1),
        1.0,
        0.0,
    )
    copies[0].wait()
    limits = [jnp.broadcast_to(sizes_ref[:, k : k + 1], (LOCAL, BD)) for k in (0, 1)]
    position = lax.broadcasted_iota(jnp.int32, (LOCAL, BD), 1)
    limit = jnp.where(position < BM, limits[0], limits[1] + BM)
    live = jnp.where(position < limit, 1.0, 0.0)
    alive[...] = live
    count = jnp.sum(live, axis=1, keepdims=True)

    for copy in copies[1:6]:
        copy.wait()
    for tile in range(36):
        columns = slice(tile * 128, tile * 128 + 128)
        flat[pl.ds(tile, LOCAL, stride=FPITCH), :] = mine_ref[:, columns]
        flat[pl.ds(36 + tile, LOCAL, stride=FPITCH), :] = theirs_ref[:, columns]
    lane = lane_index(24)
    for d in range(LOCAL):
        a = flat[pl.ds(d * FPITCH, 24, stride=3), :]
        b = flat[pl.ds(d * FPITCH + 1, 24, stride=3), :]
        c = flat[pl.ds(d * FPITCH + 2, 24, stride=3), :]
        base = d * BM
        field[pl.ds(base, 24, stride=4), :] = a
        field[pl.ds(base + 1, 24, stride=4), :] = jnp.where(
            lane < 32, pltpu.roll(a, 32, 1), pltpu.roll(b, 32, 1)
        )
        field[pl.ds(base + 2, 24, stride=4), :] = jnp.where(
            lane < 64, pltpu.roll(b, 64, 1), pltpu.roll(c, 64, 1)
        )
        field[pl.ds(base + 3, 24, stride=4), :] = pltpu.roll(c, 96, 1)

    esp = split_two(esp_ref[...])
    esp_t = split_two(left_ref[...].T)
    repulsion = 0.5 * (rep_ref[...] + rep_ref[...].T)
    half_repulsion = 0.5 * repulsion
    right = split_two(dot_three(split_two(field[...][:, 0:BM]), esp))

    def blocks(value):
        return value[0:128, 0:128], value[128:BD, 128:BD]

    def eyes():
        return eye[...], eye[0:64, 0:64]

    def diagonal_of(value):
        first_part, second_part = (
            jnp.sum(b * e, axis=0, keepdims=True) for b, e in zip(blocks(value), eyes())
        )
        return jnp.concatenate([first_part, second_part], axis=1)

    def with_diagonal(value, vector):
        (a, b), (eye_a, eye_b) = blocks(value), eyes()
        a = a + eye_a * vector[:, 0:128]
        b = b + eye_b * vector[:, 128:BD]
        return jnp.concatenate(
            [
                jnp.concatenate([a, value[0:128, 128:BD]], axis=1),
                jnp.concatenate([value[128:BD, 0:128], b], axis=1),
            ],
            axis=0,
        )

    def columns_of(value, d):
        (a, b), (eye_a, eye_b) = blocks(value), eyes()
        on_a, on_b = a * eye_a, b * eye_b
        diagonal[d : d + 1, 0:128] = jnp.sum(on_a, axis=0, keepdims=True)
        diagonal[d : d + 1, 128:BD] = jnp.sum(on_b, axis=0, keepdims=True)

        def total(part):
            return jnp.sum(jnp.abs(part), axis=0, keepdims=True)

        others[d : d + 1, 0:128] = total(a - on_a) + total(value[128:BD, 0:128])
        others[d : d + 1, 128:BD] = total(b - on_b) + total(value[0:128, 128:BD])

    copies[6].wait()
    copies[7].wait()
    for d in range(LOCAL):
        rows = slice(d * BM, d * BM + BM)
        potential = dot_three(esp_t, (right[0][rows], right[1][rows]))
        rows = slice(d * BD, d * BD + BD)
        core = jnp.concatenate([first_ref[rows, :], second_ref[rows, 0:64]], axis=1)
        total = core + potential
        total = 0.5 * (total + total.T)
        fock[d] = total
        total = total * alive[d : d + 1, :]
        total = jnp.concatenate(
            [
                jnp.where(row < limits[0][d : d + 1, :], total[0:BM], 0.0),
                jnp.where(row < limits[1][d : d + 1, :], total[BM:BD], 0.0),
            ],
            axis=0,
        )
        masked[d] = total
        columns_of(total, d)

    leaving = [pltpu.make_async_copy(fock, stack.at[0], departures.at[LOCAL])]
    leaving[0].start()

    def start(source, added):
        on_diagonal = diagonal[...] + added
        chemical = jnp.sum(on_diagonal, axis=1, keepdims=True) / count
        lowered = chemical * live
        sums = others[...] + jnp.abs(on_diagonal - lowered)
        radius = jnp.max(sums, axis=1, keepdims=True)
        scale[...] = jnp.broadcast_to(-0.5 / (radius + epsilon), (LOCAL, BD))
        shift[...] = added - lowered
        for d in range(LOCAL):
            work[d] = with_diagonal(source[d], shift[d : d + 1, :]) * scale[d : d + 1, :]

    def single(_, carry):
        for d in range(LOCAL):
            high = work[d].astype(bf16)
            work_h[d] = high
            square_h[d] = dot(high, high).astype(bf16)
        for d in range(LOCAL):
            work[d] = 1.5 * work[d] - 2.0 * dot(square_h[d], work_h[d])
        return carry

    def triple(_, carry):
        for d in range(LOCAL):
            high, low = split_two(work[d])
            work_h[d] = high
            work_l[d] = low
            squared = dot_three((high, low), (high, low))
            square_h[d], square_l[d] = split_two(squared)
        for d in range(LOCAL):
            cubed = dot_three((square_h[d], square_l[d]), (work_h[d], work_l[d]))
            work[d] = 1.5 * work[d] - 2.0 * cubed
        return carry

    def purify(singles):
        if singles > 0:
            lax.fori_loop(0, singles, single, 0)
        if singles < PURIFY:
            lax.fori_loop(singles, PURIFY, triple, 0, unroll=True)

    start(masked, jnp.zeros((LOCAL, BD), f32))
    purify(SINGLE[0])
    for d in range(LOCAL):
        occupied[d : d + 1, :] = diagonal_of(work[d])
    coulomb = dot_three(split_two(occupied[...] + 0.5 * live), split_two(repulsion))
    own_repulsion = diagonal_of(half_repulsion)
    extra[...] = live * (coulomb - 0.5 * own_repulsion)
    for d in range(LOCAL):
        changed = masked[d] - half_repulsion * work[d]
        offset[d] = changed
        columns_of(changed, d)
    start(offset, extra[...])
    purify(SINGLE[1])
    for d in range(LOCAL):
        solved = with_diagonal(work[d], 0.5 * alive[d : d + 1, :])
        density[d] = solved
        leaving.append(pltpu.make_async_copy(density.at[d], stack.at[1, d], departures.at[d]))
        leaving[-1].start()
        both = with_diagonal(masked[d] + offset[d], extra[d : d + 1, :])
        diagonal[d : d + 1, :] = jnp.sum(solved * both, axis=0, keepdims=True)
    energy = jnp.sum(diagonal[...], axis=1, keepdims=True) * (0.5 / (1024.0 * count))
    energy_out[...] = jnp.broadcast_to(jnp.sum(energy, axis=0, keepdims=True), (8, 128))
    for copy in leaving:
        copy.wait()


def solve(sizes, mine, theirs, first, second, esp_map, esp_left, repulsion):
    vmem = pl.BlockSpec(memory_space=pltpu.VMEM)
    square = (LOCAL, BD, BD)
    return pl.pallas_call(
        solve_kernel,
        name="solve",
        in_specs=[pl.BlockSpec(memory_space=pltpu.HBM)] * 8,
        out_specs=[pl.BlockSpec(memory_space=pltpu.HBM), vmem],
        out_shape=[
            jax.ShapeDtypeStruct((2,) + square, f32),
            pltpu.VMEM((8, 128), f32),
        ],
        scratch_shapes=[
            pltpu.VMEM((LOCAL, 2), jnp.int32),
            pltpu.VMEM((LOCAL, HALF), f32),
            pltpu.VMEM((LOCAL, HALF), f32),
            pltpu.VMEM((LOCAL * BD, 128), f32),
            pltpu.VMEM((LOCAL * BD, 128), f32),
            pltpu.VMEM((BM, BD), f32),
            pltpu.VMEM((BM, BD), f32),
            pltpu.VMEM((BD, BD), f32),
            pltpu.SemaphoreType.DMA((8,)),
            pltpu.VMEM(square, f32),
            pltpu.VMEM(square, f32),
            pltpu.SemaphoreType.DMA((LOCAL + 1,)),
            pltpu.VMEM((LOCAL * FPITCH, 128), f32),
            pltpu.VMEM((LOCAL * BM, 128), f32),
            pltpu.VMEM((128, 128), f32),
            pltpu.VMEM(square, f32),
            pltpu.VMEM(square, f32),
            pltpu.VMEM(square, f32),
            pltpu.VMEM(square, bf16),
            pltpu.VMEM(square, bf16),
            pltpu.VMEM(square, bf16),
            pltpu.VMEM(square, bf16),
        ]
        + [pltpu.VMEM((LOCAL, BD), f32)] * 7,
        cost_estimate=pl.CostEstimate(
            flops=11000000000, bytes_accessed=6000000, transcendentals=0
        ),
    )(sizes, mine, theirs, first, second, esp_map, esp_left, repulsion)


def esp_weights(first_ids, second_ids, centers, labels):
    middle = 0.5 * (centers[:, first_ids] + centers[:, second_ids])
    nearby = centers[:, labels]
    distance = jnp.zeros((first_ids.shape[0], labels.shape[0]), f32)
    for axis_pos in range(3):
        axis_gap = middle[axis_pos][:, None] - nearby[axis_pos][None, :]
        distance = distance + axis_gap * axis_gap
    weights = 1.0 / jnp.sqrt(distance + 1.0)
    excluded = (labels[None, :] == first_ids[:, None]) | (labels[None, :] == second_ids[:, None])
    return jnp.where(excluded, 0.0, weights)


def after(values, anchor):
    return lax.optimization_barrier((values, anchor))[0]


def on_device(
    monomer_density, monomer_centers, dimer_pairs, basis_sizes, dimer_core, esp_map, repulsion
):
    chip = lax.axis_index(GRP)
    segment = lax.axis_index("segment")

    own = lax.dynamic_slice_in_dim(monomer_density, segment * HALF, HALF, 1)
    gathered = jnp.concatenate([own] + shifts(phase_shift, own, 0), axis=0)
    blocks = [gathered] + shifts(phase_shift, gathered, 1)

    pair_ids, centers = after((dimer_pairs, monomer_centers), gathered)
    strides = [jnp.where(segment == 0, STRIDES[0][p], STRIDES[1][p]) for p in range(3)]
    places = [(chip // strides[p]) % 4 for p in range(3)]

    def moved(chips, phase, step):
        return chips + ((places[phase] + step + 4) % 4 - places[phase]) * strides[phase]

    steps = jnp.arange(4, dtype=jnp.int32)
    targets = moved(chip, 2, steps)
    rows = (jnp.arange(16, dtype=jnp.int32) + 8 * segment) % 16
    dimers = (targets[:, None] * 16 + rows[None, :]).reshape(64)
    sources = moved(moved(chip, 0, -steps)[None, :], 1, -steps[:, None])
    labels = (sources[:, :, None] * 8 + jnp.arange(8, dtype=jnp.int32)).reshape(128)
    pairs = pair_ids[:, dimers]
    weights = esp_weights(pairs[0], pairs[1], centers, labels).astype(bf16)
    parts = partial_fields(weights, blocks)

    segment_array = segment.reshape(1).astype(jnp.int32)
    core_rows, sizes_all, esp, rep = after((dimer_core, basis_sizes, esp_map, repulsion), parts[0])
    first, second, left = unflatten(segment_array, core_rows, esp)
    sizes = jnp.clip(sizes_all[pairs.reshape(2, 4, 16)[:, 0, 0:8]], 0, BM).T
    square_repulsion = rep.reshape(BD, BD)

    r0 = parts[0]
    r1, r2, r3 = shifts(lambda step: phase_shift(parts[step], 2, step))
    r1, r2, r3, first, second, sizes, esp, left, square_repulsion = lax.optimization_barrier(
        (r1, r2, r3, first, second, sizes, esp, left, square_repulsion)
    )
    own_sum, other_sum = [(r0[h] + r1[h]) + (r2[h] + r3[h]) for h in (slice(0, 8), slice(8, 16))]
    theirs = swap_cores(other_sum)
    stack, energy = solve(
        sizes, own_sum, theirs, first, second, esp, left, square_repulsion
    )

    for axis in GRP:
        one, two, three = shifts(axis_shift, energy, axis)
        energy = (energy + two) + (one + three)
    energy = energy + swap_cores(energy)
    window_energy = energy[0, 0]

    sent = flatten(jnp.stack([1 - segment, 0 * segment]).astype(jnp.int32), stack, LOCAL)
    arrived = swap_cores(sent)
    kept = flatten(jnp.stack([segment, segment]).astype(jnp.int32), stack, 2 * LOCAL)
    combined = lax.dynamic_update_slice_in_dim(kept, arrived, (1 - segment) * LOCAL, 0)
    return (combined[None], window_energy)


def solution(mesh):
    split = Mesh(
        mesh.devices.reshape(mesh.shape["segment"], 4, 4, 4), ("segment", "grp_0", "grp_1", "grp_2")
    )
    return jax.shard_map(
        on_device,
        mesh=split,
        in_specs=(P(GRP, None), P(), P(), P(), P(GRP, None), P(), P()),
        out_specs=(P("segment", GRP, None), P()),
        check_vma=False,
    )
```

```python
import jax
import jax.numpy as jnp
from jax import lax
from jax.experimental import pallas as pl
from jax.experimental.pallas import tpu as pltpu
from jax.sharding import Mesh
from jax.sharding import PartitionSpec as P


PURIFY = 8
MIB = 1024 * 1024
SINGLE = (8, 5)
GRP = ("grp_0", "grp_1", "grp_2")
ALL = ("segment", "grp_0", "grp_1", "grp_2")
STRIDES = ((1, 4, 16), (4, 16, 1))

BM = 96
BD = 192
FLAT = BD * BD
TILES = FLAT // 128
HALF = BM * BM // 2
LOCAL = 8
PITCH = 292
FPITCH = 73
epsilon = 1e-06
f32 = jnp.float32
bf16 = jnp.bfloat16


def phase_shift(value, phase, step):
    pairs = []
    for core in range(2):
        stride = STRIDES[core][phase]
        for chip in range(64):
            place = (chip // stride) % 4
            target = chip + (((place + step) % 4) - place) * stride
            pairs.append((core * 64 + chip, core * 64 + target))
    return lax.ppermute(value, ALL, pairs)


def shifts(shift, *args):
    arrived = []
    for step in (1, 2, 3):
        arrived.append(shift(*args, step))
    return arrived


def axis_shift(value, axis, step):
    return lax.ppermute(value, axis, [(i, (i + step) % 4) for i in range(4)])


def swap_cores(value):
    return lax.ppermute(value, "segment", [(0, 1), (1, 0)])


def split_two(value):
    high = value.astype(bf16)
    low = (value - high.astype(f32)).astype(bf16)
    return high, low


def dot(left, right):
    return jnp.dot(left, right, preferred_element_type=f32)


def dot_three(left, right):
    (lh, ll), (rh, rl) = left, right
    return dot(lh, rh) + (dot(ll, rh) + dot(lh, rl))


def lane_index(rows):
    return lax.broadcasted_iota(jnp.int32, (rows, 128), 1)


def unflatten_kernel(segment_ref, core_ref, esp_ref, first_ref, second_ref, left_ref, flat):
    half = BM // 2
    own = pl.multiple_of(half * segment_ref[0], 8)
    other = pl.multiple_of(half - own, 8)
    left_ref[0:half, :] = esp_ref[pl.ds(own, half), :]
    left_ref[half:BM, :] = esp_ref[pl.ds(other, half), :]
    for tile in range(TILES):
        flat[pl.ds(tile, LOCAL, stride=PITCH), :] = core_ref[:, tile * 128 : tile * 128 + 128]
    low_half = lane_index(BM) < 64
    for d in range(LOCAL):
        a = flat[pl.ds(d * PITCH, BM, stride=3), :]
        b = flat[pl.ds(d * PITCH + 1, BM, stride=3), :]
        c = flat[pl.ds(d * PITCH + 2, BM, stride=3), :]
        b_rolled = pltpu.roll(b, 64, 1)
        c_rolled = pltpu.roll(c, 64, 1)
        first_ref[pl.ds(d * BD, BM, stride=2), :] = a
        second_ref[pl.ds(d * BD, BM, stride=2), :] = b
        first_ref[pl.ds(d * BD + 1, BM, stride=2), :] = jnp.where(low_half, b_rolled, c_rolled)
        second_ref[pl.ds(d * BD + 1, BM, stride=2), :] = c_rolled


def unflatten(segment, core, esp_map):
    return pl.pallas_call(
        unflatten_kernel,
        name="unflatten",
        grid_spec=pltpu.PrefetchScalarGridSpec(
            num_scalar_prefetch=1,
            grid=(1,),
            in_specs=[
                pl.BlockSpec((LOCAL, FLAT), lambda i, s: (s[0], 0)),
                pl.BlockSpec((BM, BD), lambda i, s: (0, 0)),
            ],
            out_specs=[pl.BlockSpec((LOCAL * BD, 128), lambda i, s: (0, 0))] * 2
            + [pl.BlockSpec((BM, BD), lambda i, s: (0, 0))],
            scratch_shapes=[pltpu.VMEM((LOCAL * PITCH, 128), f32)],
        ),
        out_shape=[jax.ShapeDtypeStruct((LOCAL * BD, 128), f32)] * 2
        + [jax.ShapeDtypeStruct((BM, BD), f32)],
        cost_estimate=pl.CostEstimate(flops=20000000, bytes_accessed=3000000, transcendentals=0),
    )(segment, core, esp_map)


def flatten_kernel(place_ref, square_ref, out_ref, first, second, flat):
    low_half = lane_index(BM) < 64
    for d in range(LOCAL):
        first[...] = square_ref[0, d, :, 0:128]
        second[:, 0:64] = square_ref[0, d, :, 128:192]
        even_a = first[pl.ds(0, BM, stride=2), :]
        even_b = second[pl.ds(0, BM, stride=2), :]
        odd_a = pltpu.roll(first[pl.ds(1, BM, stride=2), :], 64, 1)
        odd_b = pltpu.roll(second[pl.ds(1, BM, stride=2), :], 64, 1)
        flat[pl.ds(d * PITCH, BM, stride=3), :] = even_a
        flat[pl.ds(d * PITCH + 1, BM, stride=3), :] = jnp.where(low_half, even_b, odd_a)
        flat[pl.ds(d * PITCH + 2, BM, stride=3), :] = jnp.where(low_half, odd_a, odd_b)
    for tile in range(TILES):
        out_ref[:, tile * 128 : tile * 128 + 128] = flat[pl.ds(tile, LOCAL, stride=PITCH), :]


def flatten(place, stack, rows):
    return pl.pallas_call(
        flatten_kernel,
        name="flatten",
        grid_spec=pltpu.PrefetchScalarGridSpec(
            num_scalar_prefetch=1,
            grid=(1,),
            in_specs=[pl.BlockSpec((1, LOCAL, BD, BD), lambda i, p: (p[0], 0, 0, 0))],
            out_specs=pl.BlockSpec((LOCAL, FLAT), lambda i, p: (p[1], 0)),
            scratch_shapes=[
                pltpu.VMEM((BD, 128), f32),
                pltpu.VMEM((BD, 128), f32),
                pltpu.VMEM((LOCAL * PITCH, 128), f32),
            ],
        ),
        out_shape=pltpu.HBM((rows, FLAT), f32),
        cost_estimate=pl.CostEstimate(flops=20000000, bytes_accessed=3000000, transcendentals=0),
    )(place, stack)


def partial_kernel(weight_ref, b0, b1, b2, b3, o0, o1, o2, o3):
    for start in range(0, HALF, 512):
        columns = slice(start, start + 512)
        rows = jnp.concatenate([b[:, columns] for b in (b0, b1, b2, b3)], axis=0)
        total = dot(weight_ref[...], rows)
        for k, out in enumerate((o0, o1, o2, o3)):
            out[:, columns] = total[16 * k : 16 * k + 16]


def partial_fields(weights, blocks):
    return pl.pallas_call(
        partial_kernel,
        name="partial_fields",
        out_shape=[pltpu.HBM((16, HALF), f32)] + [pltpu.VMEM((16, HALF), f32)] * 3,
        compiler_params=pltpu.CompilerParams(vmem_limit_bytes=12 * MIB),
        cost_estimate=pl.CostEstimate(flops=80000000, bytes_accessed=2400000, transcendentals=0),
    )(weights, *blocks)


def solve_kernel(
    sizes_any, mine_any, theirs_any, first_any, second_any, esp_any, left_any, rep_any,
    stack, energy_out,
    sizes_ref, mine_ref, theirs_ref, first_ref, second_ref, esp_ref, left_ref, rep_ref, arrivals,
    fock, density, departures, flat, field, eye, masked, offset, work, work_h, work_l, square_h, square_l,
    alive, diagonal, others, scale, shift, occupied, extra,
):
    places = (
        (sizes_any, sizes_ref), (mine_any, mine_ref), (theirs_any, theirs_ref), (esp_any, esp_ref),
        (left_any, left_ref), (rep_any, rep_ref),
        (first_any, first_ref), (second_any, second_ref),
    )
    copies = [
        pltpu.make_async_copy(source, target, arrivals.at[i])
        for i, (source, target) in enumerate(places)
    ]
    for copy in copies:
        copy.start()

    row = lax.broadcasted_iota(jnp.int32, (BM, BD), 0)
    eye[...] = jnp.where(
        lax.broadcasted_iota(jnp.int32, (128, 128), 0) == lax.broadcasted_iota(jnp.int32, (128, 128), 1),
        1.0,
        0.0,
    )
    copies[0].wait()
    limits = [jnp.broadcast_to(sizes_ref[:, k : k + 1], (LOCAL, BD)) for k in (0, 1)]
    position = lax.broadcasted_iota(jnp.int32, (LOCAL, BD), 1)
    limit = jnp.where(position < BM, limits[0], limits[1] + BM)
    live = jnp.where(position < limit, 1.0, 0.0)
    alive[...] = live
    count = jnp.sum(live, axis=1, keepdims=True)

    for copy in copies[1:6]:
        copy.wait()
    for tile in range(36):
        columns = slice(tile * 128, tile * 128 + 128)
        flat[pl.ds(tile, LOCAL, stride=FPITCH), :] = mine_ref[:, columns]
        flat[pl.ds(36 + tile, LOCAL, stride=FPITCH), :] = theirs_ref[:, columns]
    lane = lane_index(24)
    for d in range(LOCAL):
        a = flat[pl.ds(d * FPITCH, 24, stride=3), :]
        b = flat[pl.ds(d * FPITCH + 1, 24, stride=3), :]
        c = flat[pl.ds(d * FPITCH + 2, 24, stride=3), :]
        base = d * BM
        field[pl.ds(base, 24, stride=4), :] = a
        field[pl.ds(base + 1, 24, stride=4), :] = jnp.where(
            lane < 32, pltpu.roll(a, 32, 1), pltpu.roll(b, 32, 1)
        )
        field[pl.ds(base + 2, 24, stride=4), :] = jnp.where(
            lane < 64, pltpu.roll(b, 64, 1), pltpu.roll(c, 64, 1)
        )
        field[pl.ds(base + 3, 24, stride=4), :] = pltpu.roll(c, 96, 1)

    esp = split_two(esp_ref[...])
    esp_t = split_two(left_ref[...].T)
    repulsion = 0.5 * (rep_ref[...] + rep_ref[...].T)
    half_repulsion = 0.5 * repulsion
    right = split_two(dot_three(split_two(field[...][:, 0:BM]), esp))

    def blocks(value):
        return value[0:128, 0:128], value[128:BD, 128:BD]

    def eyes():
        return eye[...], eye[0:64, 0:64]

    def diagonal_of(value):
        first_part, second_part = (
            jnp.sum(b * e, axis=0, keepdims=True) for b, e in zip(blocks(value), eyes())
        )
        return jnp.concatenate([first_part, second_part], axis=1)

    def with_diagonal(value, vector):
        (a, b), (eye_a, eye_b) = blocks(value), eyes()
        a = a + eye_a * vector[:, 0:128]
        b = b + eye_b * vector[:, 128:BD]
        return jnp.concatenate(
            [
                jnp.concatenate([a, value[0:128, 128:BD]], axis=1),
                jnp.concatenate([value[128:BD, 0:128], b], axis=1),
            ],
            axis=0,
        )

    def columns_of(value, d):
        (a, b), (eye_a, eye_b) = blocks(value), eyes()
        on_a, on_b = a * eye_a, b * eye_b
        diagonal[d : d + 1, 0:128] = jnp.sum(on_a, axis=0, keepdims=True)
        diagonal[d : d + 1, 128:BD] = jnp.sum(on_b, axis=0, keepdims=True)

        def total(part):
            return jnp.sum(jnp.abs(part), axis=0, keepdims=True)

        others[d : d + 1, 0:128] = total(a - on_a) + total(value[128:BD, 0:128])
        others[d : d + 1, 128:BD] = total(b - on_b) + total(value[0:128, 128:BD])

    copies[6].wait()
    copies[7].wait()
    for d in range(LOCAL):
        rows = slice(d * BM, d * BM + BM)
        potential = dot_three(esp_t, (right[0][rows], right[1][rows]))
        rows = slice(d * BD, d * BD + BD)
        core = jnp.concatenate([first_ref[rows, :], second_ref[rows, 0:64]], axis=1)
        total = core + potential
        total = 0.5 * (total + total.T)
        fock[d] = total
        total = total * alive[d : d + 1, :]
        total = jnp.concatenate(
            [
                jnp.where(row < limits[0][d : d + 1, :], total[0:BM], 0.0),
                jnp.where(row < limits[1][d : d + 1, :], total[BM:BD], 0.0),
            ],
            axis=0,
        )
        masked[d] = total
        columns_of(total, d)

    leaving = [pltpu.make_async_copy(fock, stack.at[0], departures.at[LOCAL])]
    leaving[0].start()

    def prepare(d, value, exact):
        if exact:
            work_h[d], work_l[d] = split_two(value)
        else:
            work_h[d] = value.astype(bf16)

    def start(source, added, exact):
        on_diagonal = diagonal[...] + added
        chemical = jnp.sum(on_diagonal, axis=1, keepdims=True) / count
        lowered = chemical * live
        sums = others[...] + jnp.abs(on_diagonal - lowered)
        radius = jnp.max(sums, axis=1, keepdims=True)
        scale[...] = jnp.broadcast_to(-0.5 / (radius + epsilon), (LOCAL, BD))
        shift[...] = added - lowered
        for d in range(LOCAL):
            value = with_diagonal(source[d], shift[d : d + 1, :]) * scale[d : d + 1, :]
            work[d] = value
            prepare(d, value, exact)

    def purify(singles):
        for step in range(PURIFY):
            exact, exact_next = step >= singles, step + 1 >= singles
            for d in range(LOCAL):
                if exact:
                    pair = (work_h[d], work_l[d])
                    square_h[d], square_l[d] = split_two(dot_three(pair, pair))
                else:
                    square_h[d] = dot(work_h[d], work_h[d]).astype(bf16)
            for d in range(LOCAL):
                if exact:
                    cubed = dot_three((square_h[d], square_l[d]), (work_h[d], work_l[d]))
                else:
                    cubed = dot(square_h[d], work_h[d])
                value = 1.5 * work[d] - 2.0 * cubed
                work[d] = value
                if step + 1 < PURIFY:
                    prepare(d, value, exact_next)

    start(masked, jnp.zeros((LOCAL, BD), f32), SINGLE[0] == 0)
    purify(SINGLE[0])
    for d in range(LOCAL):
        occupied[d : d + 1, :] = diagonal_of(work[d])
    coulomb = dot_three(split_two(occupied[...] + 0.5 * live), split_two(repulsion))
    own_repulsion = diagonal_of(half_repulsion)
    extra[...] = live * (coulomb - 0.5 * own_repulsion)
    for d in range(LOCAL):
        changed = masked[d] - half_repulsion * work[d]
        offset[d] = changed
        columns_of(changed, d)
    start(offset, extra[...], SINGLE[1] == 0)
    purify(SINGLE[1])
    for d in range(LOCAL):
        solved = with_diagonal(work[d], 0.5 * alive[d : d + 1, :])
        density[d] = solved
        leaving.append(pltpu.make_async_copy(density.at[d], stack.at[1, d], departures.at[d]))
        leaving[-1].start()
        both = with_diagonal(masked[d] + offset[d], extra[d : d + 1, :])
        diagonal[d : d + 1, :] = jnp.sum(solved * both, axis=0, keepdims=True)
    energy = jnp.sum(diagonal[...], axis=1, keepdims=True) * (0.5 / (1024.0 * count))
    energy_out[...] = jnp.broadcast_to(jnp.sum(energy, axis=0, keepdims=True), (8, 128))
    for copy in leaving:
        copy.wait()


def solve(sizes, mine, theirs, first, second, esp_map, esp_left, repulsion):
    vmem = pl.BlockSpec(memory_space=pltpu.VMEM)
    square = (LOCAL, BD, BD)
    return pl.pallas_call(
        solve_kernel,
        name="solve",
        in_specs=[pl.BlockSpec(memory_space=pltpu.HBM)] * 8,
        out_specs=[pl.BlockSpec(memory_space=pltpu.HBM), vmem],
        out_shape=[
            jax.ShapeDtypeStruct((2,) + square, f32),
            pltpu.VMEM((8, 128), f32),
        ],
        scratch_shapes=[
            pltpu.VMEM((LOCAL, 2), jnp.int32),
            pltpu.VMEM((LOCAL, HALF), f32),
            pltpu.VMEM((LOCAL, HALF), f32),
            pltpu.VMEM((LOCAL * BD, 128), f32),
            pltpu.VMEM((LOCAL * BD, 128), f32),
            pltpu.VMEM((BM, BD), f32),
            pltpu.VMEM((BM, BD), f32),
            pltpu.VMEM((BD, BD), f32),
            pltpu.SemaphoreType.DMA((8,)),
            pltpu.VMEM(square, f32),
            pltpu.VMEM(square, f32),
            pltpu.SemaphoreType.DMA((LOCAL + 1,)),
            pltpu.VMEM((LOCAL * FPITCH, 128), f32),
            pltpu.VMEM((LOCAL * BM, 128), f32),
            pltpu.VMEM((128, 128), f32),
            pltpu.VMEM(square, f32),
            pltpu.VMEM(square, f32),
            pltpu.VMEM(square, f32),
            pltpu.VMEM(square, bf16),
            pltpu.VMEM(square, bf16),
            pltpu.VMEM(square, bf16),
            pltpu.VMEM(square, bf16),
        ]
        + [pltpu.VMEM((LOCAL, BD), f32)] * 7,
        cost_estimate=pl.CostEstimate(
            flops=11000000000, bytes_accessed=6000000, transcendentals=0
        ),
    )(sizes, mine, theirs, first, second, esp_map, esp_left, repulsion)


def esp_weights(first_ids, second_ids, centers, labels):
    middle = 0.5 * (centers[:, first_ids] + centers[:, second_ids])
    nearby = centers[:, labels]
    distance = jnp.zeros((first_ids.shape[0], labels.shape[0]), f32)
    for axis_pos in range(3):
        axis_gap = middle[axis_pos][:, None] - nearby[axis_pos][None, :]
        distance = distance + axis_gap * axis_gap
    weights = 1.0 / jnp.sqrt(distance + 1.0)
    excluded = (labels[None, :] == first_ids[:, None]) | (labels[None, :] == second_ids[:, None])
    return jnp.where(excluded, 0.0, weights)


def after(values, anchor):
    return lax.optimization_barrier((values, anchor))[0]


def on_device(
    monomer_density, monomer_centers, dimer_pairs, basis_sizes, dimer_core, esp_map, repulsion
):
    chip = lax.axis_index(GRP)
    segment = lax.axis_index("segment")

    own = lax.dynamic_slice_in_dim(monomer_density, segment * HALF, HALF, 1)
    gathered = jnp.concatenate([own] + shifts(phase_shift, own, 0), axis=0)
    blocks = [gathered] + shifts(phase_shift, gathered, 1)

    pair_ids, centers = after((dimer_pairs, monomer_centers), gathered)
    strides = [jnp.where(segment == 0, STRIDES[0][p], STRIDES[1][p]) for p in range(3)]
    places = [(chip // strides[p]) % 4 for p in range(3)]

    def moved(chips, phase, step):
        return chips + ((places[phase] + step + 4) % 4 - places[phase]) * strides[phase]

    steps = jnp.arange(4, dtype=jnp.int32)
    targets = moved(chip, 2, steps)
    rows = (jnp.arange(16, dtype=jnp.int32) + 8 * segment) % 16
    dimers = (targets[:, None] * 16 + rows[None, :]).reshape(64)
    sources = moved(moved(chip, 0, -steps)[None, :], 1, -steps[:, None])
    labels = (sources[:, :, None] * 8 + jnp.arange(8, dtype=jnp.int32)).reshape(128)
    pairs = pair_ids[:, dimers]
    weights = esp_weights(pairs[0], pairs[1], centers, labels).astype(bf16)
    parts = partial_fields(weights, blocks)

    segment_array = segment.reshape(1).astype(jnp.int32)
    core_rows, sizes_all, esp, rep = after((dimer_core, basis_sizes, esp_map, repulsion), parts[0])
    first, second, left = unflatten(segment_array, core_rows, esp)
    sizes = jnp.clip(sizes_all[pairs.reshape(2, 4, 16)[:, 0, 0:8]], 0, BM).T
    square_repulsion = rep.reshape(BD, BD)

    r0 = parts[0]
    r1, r2, r3 = shifts(lambda step: phase_shift(parts[step], 2, step))
    r1, r2, r3, first, second, sizes, esp, left, square_repulsion = lax.optimization_barrier(
        (r1, r2, r3, first, second, sizes, esp, left, square_repulsion)
    )
    own_sum, other_sum = [(r0[h] + r1[h]) + (r2[h] + r3[h]) for h in (slice(0, 8), slice(8, 16))]
    theirs = swap_cores(other_sum)
    stack, energy = solve(
        sizes, own_sum, theirs, first, second, esp, left, square_repulsion
    )

    for axis in GRP:
        one, two, three = shifts(axis_shift, energy, axis)
        energy = (energy + two) + (one + three)
    energy = energy + swap_cores(energy)
    window_energy = energy[0, 0]

    sent = flatten(jnp.stack([1 - segment, 0 * segment]).astype(jnp.int32), stack, LOCAL)
    arrived = swap_cores(sent)
    kept = flatten(jnp.stack([segment, segment]).astype(jnp.int32), stack, 2 * LOCAL)
    combined = lax.dynamic_update_slice_in_dim(kept, arrived, (1 - segment) * LOCAL, 0)
    return (combined[None], window_energy)


def solution(mesh):
    split = Mesh(
        mesh.devices.reshape(mesh.shape["segment"], 4, 4, 4), ("segment", "grp_0", "grp_1", "grp_2")
    )
    return jax.shard_map(
        on_device,
        mesh=split,
        in_specs=(P(GRP, None), P(), P(), P(), P(GRP, None), P(), P()),
        out_specs=(P("segment", GRP, None), P()),
        check_vma=False,
    )
```

```python
import jax
import jax.numpy as jnp
from jax import lax
from jax.experimental import pallas as pl
from jax.experimental.pallas import tpu as pltpu
from jax.sharding import Mesh
from jax.sharding import PartitionSpec as P


PURIFY = 8
MIB = 1024 * 1024
SINGLE = (8, 5)
GRP = ("grp_0", "grp_1", "grp_2")
ALL = ("segment", "grp_0", "grp_1", "grp_2")
STRIDES = ((1, 4, 16), (4, 16, 1))

BM = 96
BD = 192
FLAT = BD * BD
TILES = FLAT // 128
HALF = BM * BM // 2
LOCAL = 8
PITCH = 292
FPITCH = 73
epsilon = 1e-06
f32 = jnp.float32
bf16 = jnp.bfloat16


def phase_shift(value, phase, step):
    pairs = []
    for core in range(2):
        stride = STRIDES[core][phase]
        for chip in range(64):
            place = (chip // stride) % 4
            target = chip + ((place ^ step) - place) * stride
            pairs.append((core * 64 + chip, core * 64 + target))
    return lax.ppermute(value, ALL, pairs)


def shifts(shift, *args):
    arrived = []
    for step in (1, 2, 3):
        arrived.append(shift(*args, step))
    return arrived


def axis_shift(value, axis, step):
    return lax.ppermute(value, axis, [(i, i ^ step) for i in range(4)])


def swap_cores(value):
    return lax.ppermute(value, "segment", [(0, 1), (1, 0)])


def split_two(value):
    high = value.astype(bf16)
    low = (value - high.astype(f32)).astype(bf16)
    return high, low


def dot(left, right):
    return jnp.dot(left, right, preferred_element_type=f32)


def dot_three(left, right):
    (lh, ll), (rh, rl) = left, right
    return dot(lh, rh) + (dot(ll, rh) + dot(lh, rl))


def lane_index(rows):
    return lax.broadcasted_iota(jnp.int32, (rows, 128), 1)


def unflatten_kernel(segment_ref, core_ref, esp_ref, first_ref, second_ref, left_ref, flat):
    half = BM // 2
    own = pl.multiple_of(half * segment_ref[0], 8)
    other = pl.multiple_of(half - own, 8)
    left_ref[0:half, :] = esp_ref[pl.ds(own, half), :]
    left_ref[half:BM, :] = esp_ref[pl.ds(other, half), :]
    for tile in range(TILES):
        flat[pl.ds(tile, LOCAL, stride=PITCH), :] = core_ref[:, tile * 128 : tile * 128 + 128]
    low_half = lane_index(BM) < 64
    for d in range(LOCAL):
        a = flat[pl.ds(d * PITCH, BM, stride=3), :]
        b = flat[pl.ds(d * PITCH + 1, BM, stride=3), :]
        c = flat[pl.ds(d * PITCH + 2, BM, stride=3), :]
        b_rolled = pltpu.roll(b, 64, 1)
        c_rolled = pltpu.roll(c, 64, 1)
        first_ref[pl.ds(d * BD, BM, stride=2), :] = a
        second_ref[pl.ds(d * BD, BM, stride=2), :] = b
        first_ref[pl.ds(d * BD + 1, BM, stride=2), :] = jnp.where(low_half, b_rolled, c_rolled)
        second_ref[pl.ds(d * BD + 1, BM, stride=2), :] = c_rolled


def unflatten(segment, core, esp_map):
    return pl.pallas_call(
        unflatten_kernel,
        name="unflatten",
        grid_spec=pltpu.PrefetchScalarGridSpec(
            num_scalar_prefetch=1,
            grid=(1,),
            in_specs=[
                pl.BlockSpec((LOCAL, FLAT), lambda i, s: (s[0], 0)),
                pl.BlockSpec((BM, BD), lambda i, s: (0, 0)),
            ],
            out_specs=[pl.BlockSpec((LOCAL * BD, 128), lambda i, s: (0, 0))] * 2
            + [pl.BlockSpec((BM, BD), lambda i, s: (0, 0))],
            scratch_shapes=[pltpu.VMEM((LOCAL * PITCH, 128), f32)],
        ),
        out_shape=[jax.ShapeDtypeStruct((LOCAL * BD, 128), f32)] * 2
        + [jax.ShapeDtypeStruct((BM, BD), f32)],
        cost_estimate=pl.CostEstimate(flops=20000000, bytes_accessed=3000000, transcendentals=0),
    )(segment, core, esp_map)


def flatten_kernel(place_ref, square_ref, out_ref, first, second, flat):
    low_half = lane_index(BM) < 64
    for d in range(LOCAL):
        first[...] = square_ref[0, d, :, 0:128]
        second[:, 0:64] = square_ref[0, d, :, 128:192]
        even_a = first[pl.ds(0, BM, stride=2), :]
        even_b = second[pl.ds(0, BM, stride=2), :]
        odd_a = pltpu.roll(first[pl.ds(1, BM, stride=2), :], 64, 1)
        odd_b = pltpu.roll(second[pl.ds(1, BM, stride=2), :], 64, 1)
        flat[pl.ds(d * PITCH, BM, stride=3), :] = even_a
        flat[pl.ds(d * PITCH + 1, BM, stride=3), :] = jnp.where(low_half, even_b, odd_a)
        flat[pl.ds(d * PITCH + 2, BM, stride=3), :] = jnp.where(low_half, odd_a, odd_b)
    for tile in range(TILES):
        out_ref[:, tile * 128 : tile * 128 + 128] = flat[pl.ds(tile, LOCAL, stride=PITCH), :]


def flatten(place, stack, rows):
    return pl.pallas_call(
        flatten_kernel,
        name="flatten",
        grid_spec=pltpu.PrefetchScalarGridSpec(
            num_scalar_prefetch=1,
            grid=(1,),
            in_specs=[pl.BlockSpec((1, LOCAL, BD, BD), lambda i, p: (p[0], 0, 0, 0))],
            out_specs=pl.BlockSpec((LOCAL, FLAT), lambda i, p: (p[1], 0)),
            scratch_shapes=[
                pltpu.VMEM((BD, 128), f32),
                pltpu.VMEM((BD, 128), f32),
                pltpu.VMEM((LOCAL * PITCH, 128), f32),
            ],
        ),
        out_shape=pltpu.HBM((rows, FLAT), f32),
        cost_estimate=pl.CostEstimate(flops=20000000, bytes_accessed=3000000, transcendentals=0),
    )(place, stack)


def partial_kernel(weight_ref, b0, b1, b2, b3, o0, o1, o2, o3):
    for start in range(0, HALF, 512):
        columns = slice(start, start + 512)
        rows = jnp.concatenate([b[:, columns] for b in (b0, b1, b2, b3)], axis=0)
        total = dot(weight_ref[...], rows)
        for k, out in enumerate((o0, o1, o2, o3)):
            out[:, columns] = total[16 * k : 16 * k + 16]


def partial_fields(weights, blocks):
    return pl.pallas_call(
        partial_kernel,
        name="partial_fields",
        out_shape=[pltpu.HBM((16, HALF), f32)] + [pltpu.VMEM((16, HALF), f32)] * 3,
        compiler_params=pltpu.CompilerParams(vmem_limit_bytes=12 * MIB),
        cost_estimate=pl.CostEstimate(flops=80000000, bytes_accessed=2400000, transcendentals=0),
    )(weights, *blocks)


def solve_kernel(
    sizes_any, mine_any, theirs_any, first_any, second_any, esp_any, left_any, rep_any,
    stack, energy_out,
    sizes_ref, mine_ref, theirs_ref, first_ref, second_ref, esp_ref, left_ref, rep_ref, arrivals,
    fock, density, departures, flat, field, eye, masked, offset, work, work_h, work_l, square_h, square_l,
    alive, diagonal, others, scale, shift, occupied, extra,
):
    places = (
        (sizes_any, sizes_ref), (mine_any, mine_ref), (theirs_any, theirs_ref), (esp_any, esp_ref),
        (left_any, left_ref), (rep_any, rep_ref),
        (first_any, first_ref), (second_any, second_ref),
    )
    copies = [
        pltpu.make_async_copy(source, target, arrivals.at[i])
        for i, (source, target) in enumerate(places)
    ]
    for copy in copies:
        copy.start()

    row = lax.broadcasted_iota(jnp.int32, (BM, BD), 0)
    eye[...] = jnp.where(
        lax.broadcasted_iota(jnp.int32, (128, 128), 0) == lax.broadcasted_iota(jnp.int32, (128, 128), 1),
        1.0,
        0.0,
    )
    copies[0].wait()
    limits = [jnp.broadcast_to(sizes_ref[:, k : k + 1], (LOCAL, BD)) for k in (0, 1)]
    position = lax.broadcasted_iota(jnp.int32, (LOCAL, BD), 1)
    limit = jnp.where(position < BM, limits[0], limits[1] + BM)
    live = jnp.where(position < limit, 1.0, 0.0)
    alive[...] = live
    count = jnp.sum(live, axis=1, keepdims=True)

    for copy in copies[1:6]:
        copy.wait()
    for tile in range(36):
        columns = slice(tile * 128, tile * 128 + 128)
        flat[pl.ds(tile, LOCAL, stride=FPITCH), :] = mine_ref[:, columns]
        flat[pl.ds(36 + tile, LOCAL, stride=FPITCH), :] = theirs_ref[:, columns]
    lane = lane_index(24)
    for d in range(LOCAL):
        a = flat[pl.ds(d * FPITCH, 24, stride=3), :]
        b = flat[pl.ds(d * FPITCH + 1, 24, stride=3), :]
        c = flat[pl.ds(d * FPITCH + 2, 24, stride=3), :]
        base = d * BM
        field[pl.ds(base, 24, stride=4), :] = a
        field[pl.ds(base + 1, 24, stride=4), :] = jnp.where(
            lane < 32, pltpu.roll(a, 32, 1), pltpu.roll(b, 32, 1)
        )
        field[pl.ds(base + 2, 24, stride=4), :] = jnp.where(
            lane < 64, pltpu.roll(b, 64, 1), pltpu.roll(c, 64, 1)
        )
        field[pl.ds(base + 3, 24, stride=4), :] = pltpu.roll(c, 96, 1)

    esp = split_two(esp_ref[...])
    esp_t = split_two(left_ref[...].T)
    repulsion = 0.5 * (rep_ref[...] + rep_ref[...].T)
    half_repulsion = 0.5 * repulsion
    right = split_two(dot_three(split_two(field[...][:, 0:BM]), esp))

    def blocks(value):
        return value[0:128, 0:128], value[128:BD, 128:BD]

    def eyes():
        return eye[...], eye[0:64, 0:64]

    def diagonal_of(value):
        first_part, second_part = (
            jnp.sum(b * e, axis=0, keepdims=True) for b, e in zip(blocks(value), eyes())
        )
        return jnp.concatenate([first_part, second_part], axis=1)

    def with_diagonal(value, vector):
        (a, b), (eye_a, eye_b) = blocks(value), eyes()
        a = a + eye_a * vector[:, 0:128]
        b = b + eye_b * vector[:, 128:BD]
        return jnp.concatenate(
            [
                jnp.concatenate([a, value[0:128, 128:BD]], axis=1),
                jnp.concatenate([value[128:BD, 0:128], b], axis=1),
            ],
            axis=0,
        )

    def columns_of(value, d):
        (a, b), (eye_a, eye_b) = blocks(value), eyes()
        on_a, on_b = a * eye_a, b * eye_b
        diagonal[d : d + 1, 0:128] = jnp.sum(on_a, axis=0, keepdims=True)
        diagonal[d : d + 1, 128:BD] = jnp.sum(on_b, axis=0, keepdims=True)

        def total(part):
            return jnp.sum(jnp.abs(part), axis=0, keepdims=True)

        others[d : d + 1, 0:128] = total(a - on_a) + total(value[128:BD, 0:128])
        others[d : d + 1, 128:BD] = total(b - on_b) + total(value[0:128, 128:BD])

    copies[6].wait()
    copies[7].wait()
    for d in range(LOCAL):
        rows = slice(d * BM, d * BM + BM)
        potential = dot_three(esp_t, (right[0][rows], right[1][rows]))
        rows = slice(d * BD, d * BD + BD)
        core = jnp.concatenate([first_ref[rows, :], second_ref[rows, 0:64]], axis=1)
        total = core + potential
        total = 0.5 * (total + total.T)
        fock[d] = total
        total = total * alive[d : d + 1, :]
        total = jnp.concatenate(
            [
                jnp.where(row < limits[0][d : d + 1, :], total[0:BM], 0.0),
                jnp.where(row < limits[1][d : d + 1, :], total[BM:BD], 0.0),
            ],
            axis=0,
        )
        masked[d] = total
        columns_of(total, d)

    leaving = [pltpu.make_async_copy(fock, stack.at[0], departures.at[LOCAL])]
    leaving[0].start()

    def prepare(d, value, exact):
        if exact:
            work_h[d], work_l[d] = split_two(value)
        else:
            work_h[d] = value.astype(bf16)

    def start(source, added, exact):
        on_diagonal = diagonal[...] + added
        chemical = jnp.sum(on_diagonal, axis=1, keepdims=True) / count
        lowered = chemical * live
        sums = others[...] + jnp.abs(on_diagonal - lowered)
        radius = jnp.max(sums, axis=1, keepdims=True)
        scale[...] = jnp.broadcast_to(-0.5 / (radius + epsilon), (LOCAL, BD))
        shift[...] = added - lowered
        for d in range(LOCAL):
            value = with_diagonal(source[d], shift[d : d + 1, :]) * scale[d : d + 1, :]
            work[d] = value
            prepare(d, value, exact)

    def purify(singles):
        for step in range(PURIFY):
            exact, exact_next = step >= singles, step + 1 >= singles
            for d in range(LOCAL):
                if exact:
                    pair = (work_h[d], work_l[d])
                    square_h[d], square_l[d] = split_two(dot_three(pair, pair))
                else:
                    square_h[d] = dot(work_h[d], work_h[d]).astype(bf16)
            for d in range(LOCAL):
                if exact:
                    cubed = dot_three((square_h[d], square_l[d]), (work_h[d], work_l[d]))
                else:
                    cubed = dot(square_h[d], work_h[d])
                value = 1.5 * work[d] - 2.0 * cubed
                work[d] = value
                if step + 1 < PURIFY:
                    prepare(d, value, exact_next)

    start(masked, jnp.zeros((LOCAL, BD), f32), SINGLE[0] == 0)
    purify(SINGLE[0])
    for d in range(LOCAL):
        occupied[d : d + 1, :] = diagonal_of(work[d])
    coulomb = dot_three(split_two(occupied[...] + 0.5 * live), split_two(repulsion))
    own_repulsion = diagonal_of(half_repulsion)
    extra[...] = live * (coulomb - 0.5 * own_repulsion)
    for d in range(LOCAL):
        changed = masked[d] - half_repulsion * work[d]
        offset[d] = changed
        columns_of(changed, d)
    start(offset, extra[...], SINGLE[1] == 0)
    purify(SINGLE[1])
    for d in range(LOCAL):
        solved = with_diagonal(work[d], 0.5 * alive[d : d + 1, :])
        density[d] = solved
        leaving.append(pltpu.make_async_copy(density.at[d], stack.at[1, d], departures.at[d]))
        leaving[-1].start()
        both = with_diagonal(masked[d] + offset[d], extra[d : d + 1, :])
        diagonal[d : d + 1, :] = jnp.sum(solved * both, axis=0, keepdims=True)
    energy = jnp.sum(diagonal[...], axis=1, keepdims=True) * (0.5 / (1024.0 * count))
    energy_out[...] = jnp.broadcast_to(jnp.sum(energy, axis=0, keepdims=True), (8, 128))
    for copy in leaving:
        copy.wait()


def solve(sizes, mine, theirs, first, second, esp_map, esp_left, repulsion):
    vmem = pl.BlockSpec(memory_space=pltpu.VMEM)
    square = (LOCAL, BD, BD)
    return pl.pallas_call(
        solve_kernel,
        name="solve",
        in_specs=[pl.BlockSpec(memory_space=pltpu.HBM)] * 8,
        out_specs=[pl.BlockSpec(memory_space=pltpu.HBM), vmem],
        out_shape=[
            jax.ShapeDtypeStruct((2,) + square, f32),
            pltpu.VMEM((8, 128), f32),
        ],
        scratch_shapes=[
            pltpu.VMEM((LOCAL, 2), jnp.int32),
            pltpu.VMEM((LOCAL, HALF), f32),
            pltpu.VMEM((LOCAL, HALF), f32),
            pltpu.VMEM((LOCAL * BD, 128), f32),
            pltpu.VMEM((LOCAL * BD, 128), f32),
            pltpu.VMEM((BM, BD), f32),
            pltpu.VMEM((BM, BD), f32),
            pltpu.VMEM((BD, BD), f32),
            pltpu.SemaphoreType.DMA((8,)),
            pltpu.VMEM(square, f32),
            pltpu.VMEM(square, f32),
            pltpu.SemaphoreType.DMA((LOCAL + 1,)),
            pltpu.VMEM((LOCAL * FPITCH, 128), f32),
            pltpu.VMEM((LOCAL * BM, 128), f32),
            pltpu.VMEM((128, 128), f32),
            pltpu.VMEM(square, f32),
            pltpu.VMEM(square, f32),
            pltpu.VMEM(square, f32),
            pltpu.VMEM(square, bf16),
            pltpu.VMEM(square, bf16),
            pltpu.VMEM(square, bf16),
            pltpu.VMEM(square, bf16),
        ]
        + [pltpu.VMEM((LOCAL, BD), f32)] * 7,
        cost_estimate=pl.CostEstimate(
            flops=11000000000, bytes_accessed=6000000, transcendentals=0
        ),
    )(sizes, mine, theirs, first, second, esp_map, esp_left, repulsion)


def esp_weights(first_ids, second_ids, centers, labels):
    middle = 0.5 * (centers[:, first_ids] + centers[:, second_ids])
    nearby = centers[:, labels]
    distance = jnp.zeros((first_ids.shape[0], labels.shape[0]), f32)
    for axis_pos in range(3):
        axis_gap = middle[axis_pos][:, None] - nearby[axis_pos][None, :]
        distance = distance + axis_gap * axis_gap
    weights = 1.0 / jnp.sqrt(distance + 1.0)
    excluded = (labels[None, :] == first_ids[:, None]) | (labels[None, :] == second_ids[:, None])
    return jnp.where(excluded, 0.0, weights)


def after(values, anchor):
    return lax.optimization_barrier((values, anchor))[0]


def on_device(
    monomer_density, monomer_centers, dimer_pairs, basis_sizes, dimer_core, esp_map, repulsion
):
    chip = lax.axis_index(GRP)
    segment = lax.axis_index("segment")

    own = lax.dynamic_slice_in_dim(monomer_density, segment * HALF, HALF, 1)
    gathered = jnp.concatenate([own] + shifts(phase_shift, own, 0), axis=0)
    blocks = [gathered] + shifts(phase_shift, gathered, 1)

    pair_ids, centers = after((dimer_pairs, monomer_centers), gathered)
    strides = [jnp.where(segment == 0, STRIDES[0][p], STRIDES[1][p]) for p in range(3)]
    places = [(chip // strides[p]) % 4 for p in range(3)]

    def moved(chips, phase, step):
        return chips + ((places[phase] ^ step) - places[phase]) * strides[phase]

    steps = jnp.arange(4, dtype=jnp.int32)
    targets = moved(chip, 2, steps)
    rows = (jnp.arange(16, dtype=jnp.int32) + 8 * segment) % 16
    dimers = (targets[:, None] * 16 + rows[None, :]).reshape(64)
    sources = moved(moved(chip, 0, steps)[None, :], 1, steps[:, None])
    labels = (sources[:, :, None] * 8 + jnp.arange(8, dtype=jnp.int32)).reshape(128)
    pairs = pair_ids[:, dimers]
    weights = esp_weights(pairs[0], pairs[1], centers, labels).astype(bf16)
    parts = partial_fields(weights, blocks)

    segment_array = segment.reshape(1).astype(jnp.int32)
    core_rows, sizes_all, esp, rep = after((dimer_core, basis_sizes, esp_map, repulsion), parts[0])
    first, second, left = unflatten(segment_array, core_rows, esp)
    sizes = jnp.clip(sizes_all[pairs.reshape(2, 4, 16)[:, 0, 0:8]], 0, BM).T
    square_repulsion = rep.reshape(BD, BD)

    r0 = parts[0]
    r1, r2, r3 = shifts(lambda step: phase_shift(parts[step], 2, step))
    r1, r2, r3, first, second, sizes, esp, left, square_repulsion = lax.optimization_barrier(
        (r1, r2, r3, first, second, sizes, esp, left, square_repulsion)
    )
    own_sum, other_sum = [(r0[h] + r1[h]) + (r2[h] + r3[h]) for h in (slice(0, 8), slice(8, 16))]
    theirs = swap_cores(other_sum)
    stack, energy = solve(
        sizes, own_sum, theirs, first, second, esp, left, square_repulsion
    )

    for axis in GRP:
        one, two, three = shifts(axis_shift, energy, axis)
        energy = (energy + two) + (one + three)
    energy = energy + swap_cores(energy)
    window_energy = energy[0, 0]

    sent = flatten(jnp.stack([1 - segment, 0 * segment]).astype(jnp.int32), stack, LOCAL)
    arrived = swap_cores(sent)
    kept = flatten(jnp.stack([segment, segment]).astype(jnp.int32), stack, 2 * LOCAL)
    combined = lax.dynamic_update_slice_in_dim(kept, arrived, (1 - segment) * LOCAL, 0)
    return (combined[None], window_energy)


def solution(mesh):
    split = Mesh(
        mesh.devices.reshape(mesh.shape["segment"], 4, 4, 4), ("segment", "grp_0", "grp_1", "grp_2")
    )
    return jax.shard_map(
        on_device,
        mesh=split,
        in_specs=(P(GRP, None), P(), P(), P(), P(GRP, None), P(), P()),
        out_specs=(P("segment", GRP, None), P()),
        check_vma=False,
    )
```
